32 devices in a mesh: dp: 4 (over y, x), seq: 4 (over z), tensor: 2 (over core).
Axes of the slice: x: 2, y: 2, z: 4, core: 2. Of those that a mesh axis runs over, the one named last changes fastest.
Arguments:
- pixels: bfloat16 [4, 1568, 1536], P('dp', 'seq'), may hold values from -6 to 6
- visible: int32 [4, 157], P('dp'), may hold values from 0 to 1567, as said below
- micro_of: int32 [4], replicated, may hold values from 0 to 1, as said below
- encoder_weights: bfloat16 [3, 768, 3072], P(None, ('dp', 'seq'), 'tensor')
- decoder_weights: bfloat16 [4, 384, 1536], P(None, ('dp', 'seq'), 'tensor')
- border_weights: bfloat16 [768, 1920], P(('dp', 'seq')), may hold values from -0.21875 to 0.21875
- vector_params: bfloat16 [384, 10], P(('dp', 'seq'))
- encoder_mean: float32 [3, 768, 3072], P(None, ('dp', 'seq'), 'tensor'), may hold values from -4.7683716e-06 to 4.7683716e-06
- decoder_mean: float32 [4, 384, 1536], P(None, ('dp', 'seq'), 'tensor'), may hold values from -4.7683716e-06 to 4.7683716e-06
- border_mean: float32 [768, 1920], P(('dp', 'seq')), may hold values from -4.7683716e-06 to 4.7683716e-06
- vector_mean: float32 [384, 10], P(('dp', 'seq')), may hold values from -4.7683716e-06 to 4.7683716e-06
- encoder_square: float32 [3, 768, 3072], P(None, ('dp', 'seq'), 'tensor'), may hold values from 2e-14 to 1e-13
- decoder_square: float32 [4, 384, 1536], P(None, ('dp', 'seq'), 'tensor'), may hold values from 2e-14 to 1e-13
- border_square: float32 [768, 1920], P(('dp', 'seq')), may hold values from 2e-14 to 1e-13
- vector_square: float32 [384, 10], P(('dp', 'seq')), may hold values from 2e-14 to 1e-13
Outputs:
- encoder_mean_next: float32 [3, 768, 3072], P(None, ('dp', 'seq'), 'tensor')
- encoder_square_next: float32 [3, 768, 3072], P(None, ('dp', 'seq'), 'tensor')
- encoder_update: float32 [3, 768, 3072], P(None, ('dp', 'seq'), 'tensor')
- decoder_mean_next: float32 [4, 384, 1536], P(None, ('dp', 'seq'), 'tensor')
- decoder_square_next: float32 [4, 384, 1536], P(None, ('dp', 'seq'), 'tensor')
- decoder_update: float32 [4, 384, 1536], P(None, ('dp', 'seq'), 'tensor')
- border_mean_next: float32 [768, 1920], P(('dp', 'seq'))
- border_square_next: float32 [768, 1920], P(('dp', 'seq'))
- border_update: float32 [768, 1920], P(('dp', 'seq'))
- vector_mean_next: float32 [384, 10], P(('dp', 'seq'))
- vector_square_next: float32 [384, 10], P(('dp', 'seq'))
- vector_update: float32 [384, 10], P(('dp', 'seq'))
- losses: float32 [2], replicated
- grad_norm: float32 [1], replicated
The draws below stay inside these ranges and needn't reach their ends.
Inputs may be any that keep to these rules, and one draw needn't show every extreme that they name: `visible`: each row names 157 different tubes. `micro_of`: each micro-batch holds at least one clip.
All inputs are finite; a program needn't handle non-finite values.
Results may differ from the reference program's by a relative error of at most 0.017.
Values may be sent and summed in bfloat16 or wider, within the bound.
A program may use at most 128 MiB of HBM per device.

```python
import math
import jax
import jax.numpy as jnp
from jax import lax

PIX = 1536
D = 768
HEADS = 12
HD = 64
FF = 3072
DD = 384
DHEADS = 6
DFF = 1536
TUBES = 1568
VIS = 157
MICRO = 2
CLIPS = 4
VCOLS = 10


def draw_visible(key, part):

    def one_clip(clip_number):
        subkey = jax.random.fold_in(jax.random.fold_in(key, 11), clip_number)
        shuffled = jax.random.permutation(subkey, TUBES - 1)[:VIS].astype(jnp.int32)
        first_slot = jnp.arange(VIS, dtype=jnp.int32) == 0
        return jnp.where((clip_number == 0) & first_slot, jnp.int32(TUBES - 1), shuffled)
    return jax.vmap(one_clip)(jnp.arange(CLIPS, dtype=jnp.int32))


def draw_micro_of(key, part):
    first, second = jax.random.split(jax.random.fold_in(key, 7))
    cutoff = jax.random.randint(first, (), 1, CLIPS)
    shuffled = jax.random.permutation(second, CLIPS)
    return (shuffled < cutoff).astype(jnp.int32)


def draw_encoder_weights(key, part):
    normal_draw = jax.random.normal(key, (3, D, FF), jnp.float32)
    column = jnp.arange(FF) % (4 * HD)
    attn_scale = jnp.where(column < 3 * HD, 1.0, 0.5 * VIS ** 0.5) * D ** (-0.5)
    scales = jnp.stack([attn_scale, jnp.full((FF,), D ** (-0.5)), jnp.full((FF,), 2.0 * FF ** (-0.5))])
    return (normal_draw * scales[:, None, :]).astype(jnp.bfloat16)


def draw_decoder_weights(key, part):
    normal_draw = jax.random.normal(key, (4, DD, DFF), jnp.float32)
    column = jnp.arange(DFF) % (4 * HD)
    attn_scale = jnp.where(column < 3 * HD, 1.0, 0.5 * TUBES ** 0.5) * DD ** (-0.5)
    scales = jnp.stack([attn_scale, jnp.full((DFF,), DD ** (-0.5)), jnp.full((DFF,), 2.0 * DFF ** (-0.5)), jnp.full((DFF,), DD ** (-0.5))])
    return (normal_draw * scales[:, None, :]).astype(jnp.bfloat16)


def draw_vector_params(key, part):
    first, second = jax.random.split(jax.random.fold_in(key, 5))
    gains = 1.0 + 0.3 * jax.random.uniform(first, (DD, VCOLS), jnp.float32, -1.0, 1.0)
    mask_token = jax.random.normal(second, (DD, VCOLS), jnp.float32)
    column = jnp.arange(VCOLS)
    return jnp.where(column[None, :] == VCOLS - 1, mask_token, gains).astype(jnp.bfloat16)


def shard_levels(stream_key, shape, pieces, smallest, high):
    loudness = 1.0
    for axis_at, shards_of in pieces:
        draws = jax.random.uniform(jax.random.fold_in(jax.random.fold_in(stream_key, 6), axis_at), (shards_of,), jnp.float32, smallest / len(pieces), high / len(pieces))
        loudness = loudness * jnp.repeat(jnp.exp(draws), shape[axis_at] // shards_of).reshape((-1,) + (1,) * (len(shape) - 1 - axis_at))
    return loudness


def normal_values(own_key, shape, width, most, cuts=(), held_as=jnp.bfloat16):
    values = width * jax.random.normal(own_key, shape, jnp.float32)
    if cuts:
        values = values * shard_levels(own_key, shape, cuts, -0.22, 0.18)
    return jnp.clip(values, -most, most).astype(held_as)


def setup_inputs(seed: int = 0) -> dict:
    arg_keys = jax.random.split(jax.random.key(seed), 16)
    pixels = normal_values(arg_keys[0], (CLIPS, TUBES, PIX), 1.0, 6.0, ((0, 4), (1, 4)))
    visible = draw_visible(jax.random.fold_in(arg_keys[15], 71), 0)
    micro_of = draw_micro_of(jax.random.fold_in(arg_keys[15], 71), 0)
    encoder_weights = draw_encoder_weights(jax.random.fold_in(arg_keys[15], 71), 0)
    decoder_weights = draw_decoder_weights(jax.random.fold_in(arg_keys[15], 71), 0)
    border_weights = normal_values(arg_keys[5], (D, PIX + DD), D ** -0.5, 0.21875, ((0, 16),))
    vector_params = draw_vector_params(jax.random.fold_in(arg_keys[15], 71), 0)
    encoder_mean = normal_values(arg_keys[7], (3, D, FF), (8e-7), 4.76837158203125e-06, ((1, 16), (2, 2)), jnp.float32)
    decoder_mean = normal_values(arg_keys[8], (4, DD, DFF), (8e-7), 4.76837158203125e-06, ((1, 16), (2, 2)), jnp.float32)
    border_mean = normal_values(arg_keys[9], (D, PIX + DD), (8e-7), 4.76837158203125e-06, ((0, 16),), jnp.float32)
    vector_mean = normal_values(arg_keys[10], (DD, VCOLS), (8e-7), 4.76837158203125e-06, ((0, 16),), jnp.float32)
    encoder_square = jnp.clip(jnp.exp(math.log(9.9999998245167e-14) - 1.609438 * jax.random.uniform(arg_keys[11], (3, D, FF), jnp.float32) ** shard_levels(arg_keys[11], (3, D, FF), ((1, 16), (2, 2)), -0.2, 0.2)), 1.99999996490334e-14, 9.9999998245167e-14)
    decoder_square = jnp.clip(jnp.exp(math.log(9.9999998245167e-14) - 1.609438 * jax.random.uniform(arg_keys[12], (4, DD, DFF), jnp.float32) ** shard_levels(arg_keys[12], (4, DD, DFF), ((1, 16), (2, 2)), -0.2, 0.2)), 1.99999996490334e-14, 9.9999998245167e-14)
    border_square = jnp.clip(jnp.exp(math.log(9.9999998245167e-14) - 1.609438 * jax.random.uniform(arg_keys[13], (D, PIX + DD), jnp.float32) ** shard_levels(arg_keys[13], (D, PIX + DD), ((0, 16),), -0.2, 0.2)), 1.99999996490334e-14, 9.9999998245167e-14)
    vector_square = jnp.clip(jnp.exp(math.log(9.9999998245167e-14) - 1.609438 * jax.random.uniform(arg_keys[14], (DD, VCOLS), jnp.float32) ** shard_levels(arg_keys[14], (DD, VCOLS), ((0, 16),), -0.2, 0.2)), 1.99999996490334e-14, 9.9999998245167e-14)
    return {"pixels": pixels, "visible": visible, "micro_of": micro_of, "encoder_weights": encoder_weights, "decoder_weights": decoder_weights, "border_weights": border_weights, "vector_params": vector_params, "encoder_mean": encoder_mean, "decoder_mean": decoder_mean, "border_mean": border_mean, "vector_mean": vector_mean, "encoder_square": encoder_square, "decoder_square": decoder_square, "border_square": border_square, "vector_square": vector_square}


HIGH = lax.Precision.HIGHEST
EPS_NORM = 1e-06
CLIP_LIMIT = 0.025
LEARN_RATE = 0.01
WEIGHT_DECAY = 0.05
BETA_FIRST = 0.9
BETA_SECOND = 0.999
ADAM_EPS = 1e-08
BIAS_STEP = 10.0

@jax.custom_vjp
def low(v):
    return lax.optimization_barrier(v.astype(jnp.bfloat16)).astype(jnp.float32)

@jax.custom_vjp
def low_back(v):
    return v

def low_keep(v):
    return (low(v), None)

def low_pass(kept, grad):
    return (grad,)

def back_keep(v):
    return (v, None)

def back_low(kept, grad):
    return (low(grad),)
low.defvjp(low_keep, low_pass)
low_back.defvjp(back_keep, back_low)

def round_both(v):
    return low(low_back(v))

def layer_norm(x, norm_gain):
    row_mean = lax.optimization_barrier(jnp.mean(x, axis=-1, keepdims=True))
    centred = x - row_mean
    variance = lax.optimization_barrier(jnp.mean(centred * centred, axis=-1, keepdims=True))
    return centred * lax.rsqrt(variance + EPS_NORM) * norm_gain

def sinusoid(positions, model_width):
    half_width = model_width // 2
    frequency = jnp.exp(jnp.arange(half_width, dtype=jnp.float32) * (-math.log(10000.0) / half_width))
    angles = positions.astype(jnp.float32)[:, None] * frequency[None, :]
    return jnp.concatenate([jnp.sin(angles), jnp.cos(angles)], axis=1)

def gelu_exact(v):
    return jax.nn.gelu(v, approximate=False)

def attend(x, weights, norm_gain, head_count):
    model_width = x.shape[1]
    blocks = weights.reshape(model_width, head_count, 4, HD)
    normed = low(layer_norm(x, norm_gain))
    query_rows = round_both(jnp.einsum('td,dhe->hte', normed, blocks[:, :, 0, :], precision=HIGH))
    key_rows = round_both(jnp.einsum('td,dhe->hte', normed, blocks[:, :, 1, :], precision=HIGH))
    value_rows = round_both(jnp.einsum('td,dhe->hte', normed, blocks[:, :, 2, :], precision=HIGH))
    scores = low_back(jnp.einsum('hte,hse->hts', query_rows, key_rows, precision=HIGH) * HD ** (-0.5))
    softmaxed = low(jax.nn.softmax(scores, axis=-1))
    mixture = round_both(jnp.einsum('hts,hse->hte', softmaxed, value_rows, precision=HIGH))
    branch = jnp.einsum('hte,dhe->td', mixture, blocks[:, :, 3, :], precision=HIGH)
    return x + low_back(branch)

def feed_forward(x, up_proj, down_proj, norm_gain):
    normed = low(layer_norm(x, norm_gain))
    preact = low_back(jnp.dot(normed, up_proj, precision=HIGH))
    activation = low(gelu_exact(preact))
    return x + low_back(jnp.dot(activation, down_proj.T, precision=HIGH))

def clip_loss(params, clip_pixels, visible_row, weight):
    encoder, decoder, border, vector = params
    width_ratio = D // DD
    gain_list = [vector[:, 0:width_ratio].reshape(D), vector[:, width_ratio:2 * width_ratio].reshape(D), vector[:, 2 * width_ratio:3 * width_ratio].reshape(D), vector[:, 3 * width_ratio], vector[:, 3 * width_ratio + 1], vector[:, 3 * width_ratio + 2]]
    mask_token = vector[:, 3 * width_ratio + 3]
    seen_pixels = clip_pixels[visible_row]
    x = low_back(jnp.einsum('vp,dp->vd', seen_pixels, border[:, :PIX], precision=HIGH)) + sinusoid(visible_row, D)
    x = attend(x, encoder[0], gain_list[0], HEADS)
    x = feed_forward(x, encoder[1], encoder[2], gain_list[1])
    normed = low(layer_norm(x, gain_list[2]))
    latent = low_back(jnp.dot(normed, border[:, PIX:], precision=HIGH))
    placed = jnp.zeros((TUBES, DD), latent.dtype).at[visible_row].set(latent)
    visible_flag = jnp.zeros((TUBES,), jnp.int32).at[visible_row].set(1)
    z = jnp.where(visible_flag[:, None] == 1, placed, mask_token[None, :]) + sinusoid(jnp.arange(TUBES, dtype=jnp.int32), DD)
    z = attend(z, decoder[0], gain_list[3], DHEADS)
    z = feed_forward(z, decoder[1], decoder[2], gain_list[4])
    final_norm = low(layer_norm(z, gain_list[5]))
    prediction = low_back(jnp.dot(final_norm, decoder[3], precision=HIGH))
    residue = prediction - clip_pixels
    return weight * jnp.sum(jnp.where(visible_flag[:, None] == 1, 0.0, residue * residue))

def adam_update(gradient, weights, mean_old, square_old, factor):
    scaled = gradient * factor
    mean_next = BETA_FIRST * mean_old + (1.0 - BETA_FIRST) * scaled
    square_next = BETA_SECOND * square_old + (1.0 - BETA_SECOND) * scaled * scaled
    first_fix = 1.0 - BETA_FIRST ** BIAS_STEP
    second_fix = 1.0 - BETA_SECOND ** BIAS_STEP
    update = -LEARN_RATE * (mean_next / first_fix / (jnp.sqrt(square_next / second_fix) + ADAM_EPS) + WEIGHT_DECAY * weights.astype(jnp.float32))
    return (mean_next, square_next, update)

def reference(pixels, visible, micro_of, encoder_weights, decoder_weights, border_weights, vector_params, encoder_mean, decoder_mean, border_mean, vector_mean, encoder_square, decoder_square, border_square, vector_square):
    params = tuple((w.astype(jnp.float32) for w in (encoder_weights, decoder_weights, border_weights, vector_params)))
    micro_slots = jnp.arange(MICRO, dtype=jnp.int32)
    counts = lax.optimization_barrier(jnp.sum((micro_of[:, None] == micro_slots[None, :]).astype(jnp.float32), axis=0))

    def per_clip(carry, inputs):
        gradients, losses = carry
        clip_pixels, visible_row, micro_index = inputs
        weight = 1.0 / (counts[micro_index] * float(MICRO * (TUBES - VIS) * PIX))

        def loss_of(*p):
            return clip_loss(p, clip_pixels.astype(jnp.float32), visible_row, weight)
        loss_value, pullback = jax.vjp(loss_of, *params)
        clip_grads = pullback(jnp.ones_like(loss_value))
        gradients = tuple((g + q for g, q in zip(gradients, clip_grads)))
        losses = losses + loss_value * (micro_slots == micro_index).astype(loss_value.dtype)
        return ((gradients, losses), None)
    initial = (tuple((jnp.zeros_like(p) for p in params)), jnp.zeros((MICRO,), jnp.float32))
    (gradients, losses), unused = lax.scan(per_clip, initial, (pixels, visible, micro_of))
    square_sum = sum((jnp.sum(g * g) for g in gradients))
    grad_norm = jnp.sqrt(square_sum)
    factor = jnp.minimum(1.0, CLIP_LIMIT / grad_norm)
    enc_next = adam_update(gradients[0], encoder_weights, encoder_mean, encoder_square, factor)
    dec_next = adam_update(gradients[1], decoder_weights, decoder_mean, decoder_square, factor)
    bor_next = adam_update(gradients[2], border_weights, border_mean, border_square, factor)
    vec_next = adam_update(gradients[3], vector_params, vector_mean, vector_square, factor)
    return (enc_next[0], enc_next[1], enc_next[2], dec_next[0], dec_next[1], dec_next[2], bor_next[0], bor_next[1], bor_next[2], vec_next[0], vec_next[1], vec_next[2], losses, jnp.reshape(grad_norm, (1,)))
```

```python
import math

import jax
import jax.numpy as jnp
from jax import lax
from jax.experimental import pallas as pl
from jax.experimental.pallas import tpu as pltpu
from jax.sharding import PartitionSpec as P

PIX = 1536
D = 768
HD = 64
DD = 384
TUBES = 1568
VIS = 157
MICRO = 2


HIGH = lax.Precision.HIGHEST
EPS_NORM = 1e-06
CLIP_LIMIT = 0.025
LEARN_RATE = 0.01
WEIGHT_DECAY = 0.05
BETA_FIRST = 0.9
BETA_SECOND = 0.999
ADAM_EPS = 1e-08
BIAS_STEP = 10.0


MESH_ID = pl.DeviceIdType.MESH


def flip_low(d):
    return d + 1 - 2 * (d % 2)


def flip_high(d):
    return (d + 2) % 4


def line_neighbours(s):
    return 1 - s // 3 + (s + 2) // 3


def send(source, target, send_sem, recv_sem, device):
    copy = pltpu.make_async_remote_copy(
        src_ref=source,
        dst_ref=target,
        send_sem=send_sem,
        recv_sem=recv_sem,
        device_id=device,
        device_id_type=MESH_ID,
    )
    copy.start()


def wait_got(place, recv_sem):
    pltpu.make_async_copy(place, place, recv_sem).wait()


def greet(devices):
    barrier = pltpu.get_barrier_semaphore()
    for device in devices:
        pl.semaphore_signal(barrier, inc=1, device_id=device, device_id_type=MESH_ID)
    return barrier


def gather_kernel(enc, dec, bor, vec, pix, enc_o, dec_o, bor_o, vec_o, pix_o, send_sem, recv_sem, pair_send, pair_recv, own_sem):
    d = lax.axis_index("dp")
    s = lax.axis_index("seq")
    t = lax.axis_index("tensor")
    rows = enc.shape[1]
    small = dec.shape[1]
    part = rows // 2
    near = {"dp": flip_low(d)}
    far = {"dp": flip_high(d)}
    up = {"seq": s + 1}
    down = {"seq": s - 1}
    mate = {"tensor": 1 - t}
    d_near = flip_low(d)
    d_far = flip_high(d)
    d_diag = 3 - d

    def enc_place(m, c0, w):
        def at(viewer, dd, ss):
            slot = ((ss - viewer + 4) % 4) * 4 + dd
            return enc_o.at[m, pl.ds(pl.multiple_of(slot * rows, 8), rows), c0 : c0 + w]
        return (enc.at[m, :, c0 : c0 + w], at)

    def bor_place(c0, w):
        def at(viewer, dd, ss):
            slot = ((ss - viewer + 4) % 4) * 4 + dd
            return bor_o.at[pl.ds(pl.multiple_of(slot * rows + t * part, 8), part), c0 : c0 + w]
        return (bor.at[pl.ds(pl.multiple_of(t * part, 8), part), c0 : c0 + w], at)

    def dec_place(m):
        def at(viewer, dd, ss):
            return dec_o.at[m, pl.ds(pl.multiple_of((dd * 4 + ss) * small, 8), small), :]
        return (dec.at[m], at)

    def vec_place():
        def at(viewer, dd, ss):
            return vec_o.at[dd * 4 + ss]
        return (vec, at)

    def pix_place():
        half = pix.shape[1] // 2
        cols = pl.ds(pl.multiple_of(t * half, 128), half)
        def at(viewer, dd, ss):
            return pix_o.at[ss, :, cols]
        return (pix.at[:, cols], at)

    pieces = [
        (0, False, vec_place()),
        (2, True, pix_place()),
        (0, True, bor_place(0, 768)),
        (1, True, bor_place(768, 768)),
        (0, False, enc_place(0, 0, 768)),
        (1, False, enc_place(0, 768, 768)),
        (0, False, enc_place(1, 0, 768)),
        (1, False, enc_place(1, 768, 768)),
        (0, False, enc_place(2, 0, 768)),
        (1, False, enc_place(2, 768, 768)),
        (0, True, bor_place(1536, 384)),
        (1, False, dec_place(0)),
        (0, False, dec_place(1)),
        (1, False, dec_place(2)),
        (0, False, dec_place(3)),
    ]
    paired = [p for p in range(len(pieces)) if pieces[p][1]]

    barrier = greet([near, far, mate])
    @pl.when(s < 3)
    def _():
        pl.semaphore_signal(barrier, inc=1, device_id=up, device_id_type=MESH_ID)
    @pl.when(s > 0)
    def _():
        pl.semaphore_signal(barrier, inc=1, device_id=down, device_id_type=MESH_ID)
    pl.semaphore_wait(barrier, 3 + line_neighbours(s))

    def hops(kind):
        return (near, far) if kind == 0 else (far, near)

    for p, (kind, pair, (own, at)) in enumerate(pieces):
        got = recv_sem.at[p, d * 4 + s]
        @pl.when(s < 3)
        def _():
            send(own, at(s + 1, d, s), send_sem.at[p, 0], got, up)
        @pl.when(s > 0)
        def _():
            send(own, at(s - 1, d, s), send_sem.at[p, 4], got, down)
        if kind != 2:
            first, second = hops(kind)
            send(own, at(s, d, s), send_sem.at[p, 5], got, first)
            send(own, at(s, d, s), send_sem.at[p, 9], got, second)
    own_copies = [
        (enc, enc_o.at[:, pl.ds(pl.multiple_of(d * rows, 8), rows), :]),
        (dec, dec_o.at[:, pl.ds(pl.multiple_of((d * 4 + s) * small, 8), small), :]),
        (bor, bor_o.at[pl.ds(pl.multiple_of(d * rows, 8), rows), :]),
        (vec, vec_o.at[d * 4 + s]),
        (pix, pix_o.at[s]),
    ]
    for j, (source, target) in enumerate(own_copies):
        pltpu.make_async_copy(source, target, own_sem.at[j]).start()

    def to_mate(p, at, dd, ss):
        if pieces[p][1]:
            q = paired.index(p)
            place = at(s, dd, ss)
            send(place, place, pair_send.at[q, dd * 4 + ss], pair_recv.at[q, dd * 4 + ss], mate)

    def column(p):
        kind, pair, (own, at) = pieces[p]
        for k in range(1, 4):
            for sign in (-1, 1):
                ss = s + sign * k
                @pl.when((ss >= 0) & (ss <= 3))
                def _():
                    place = at(s, d, ss)
                    got = recv_sem.at[p, d * 4 + ss]
                    wait_got(place, got)
                    if k < 3:
                        if sign < 0:
                            @pl.when(s < 3)
                            def _():
                                send(place, at(s + 1, d, ss), send_sem.at[p, k], got, up)
                        else:
                            @pl.when(s > 0)
                            def _():
                                send(place, at(s - 1, d, ss), send_sem.at[p, 16 + k], got, down)
                    if kind != 2:
                        first, second = hops(kind)
                        send(place, place, send_sem.at[p, 5 + (ss - s + 4) % 4], got, first)
                        send(place, place, send_sem.at[p, 9 + (ss - s + 4) % 4], got, second)
                    to_mate(p, at, d, ss)

    def plane(p):
        kind, pair, (own, at) = pieces[p]
        if kind == 2:
            return
        dd = d_near if kind == 0 else d_far
        second = hops(kind)[1]
        for k in range(0, 4):
            for sign in (-1, 1) if k else (1,):
                ss = s + sign * k
                @pl.when((ss >= 0) & (ss <= 3))
                def _():
                    place = at(s, dd, ss)
                    got = recv_sem.at[p, dd * 4 + ss]
                    wait_got(place, got)
                    send(place, place, send_sem.at[p, 13 + (ss - s + 4) % 4], got, second)
                    to_mate(p, at, dd, ss)

    def last(p):
        kind, pair, (own, at) = pieces[p]
        if kind == 2:
            return
        for dd in (d_far, d_diag) if kind == 0 else (d_near, d_diag):
            for k in range(0, 4):
                for sign in (-1, 1) if k else (1,):
                    ss = s + sign * k
                    @pl.when((ss >= 0) & (ss <= 3))
                    def _():
                        place = at(s, dd, ss)
                        wait_got(place, recv_sem.at[p, dd * 4 + ss])
                        to_mate(p, at, dd, ss)

    def drain(p):
        kind, pair, (own, at) = pieces[p]
        def sent(slot):
            wait_got(own, send_sem.at[p, slot])
        @pl.when(s < 3)
        def _():
            sent(0)
        @pl.when(s > 0)
        def _():
            sent(4)
        for k in (1, 2):
            @pl.when((s - k >= 0) & (s < 3))
            def _():
                sent(k)
            @pl.when((s + k <= 3) & (s > 0))
            def _():
                sent(16 + k)
        if kind != 2:
            for slot in range(5, 17):
                sent(slot)
        if pair:
            q = paired.index(p)
            t_other = 1 - t
            for dd in (d, d_near, d_far, d_diag):
                for ss_rel in range(4):
                    ss = (s + ss_rel) % 4
                    if ss_rel == 0 and dd is d:
                        continue
                    if kind == 2 and dd is not d:
                        continue
                    wait_got(own, pair_send.at[q, dd * 4 + ss])
                    wait_got(own, pair_recv.at[q, dd * 4 + ss])

    count = len(pieces)
    for p in range(count):
        column(p)
        if p >= 1:
            plane(p - 1)
        if p >= 3:
            last(p - 3)
    plane(count - 1)
    for p in range(count - 3, count):
        last(p)
    for p in range(count):
        drain(p)
    for j, (source, target) in enumerate(own_copies):
        pltpu.make_async_copy(source, target, own_sem.at[j]).wait()


def gather_all(encoder_weights, decoder_weights, border_weights, vec_tile, pixel_rows):
    rows = encoder_weights.shape[1]
    small = decoder_weights.shape[1]
    hbm = pl.BlockSpec(memory_space=pl.ANY)
    vmem = pl.BlockSpec(memory_space=pltpu.VMEM)
    count = 15
    return pl.pallas_call(
        gather_kernel,
        out_shape=(
            jax.ShapeDtypeStruct((3, rows * 16, encoder_weights.shape[2]), jnp.bfloat16),
            jax.ShapeDtypeStruct((4, small * 16, decoder_weights.shape[2]), jnp.bfloat16),
            jax.ShapeDtypeStruct((rows * 16, border_weights.shape[1]), jnp.bfloat16),
            jax.ShapeDtypeStruct((16,) + vec_tile.shape, jnp.float32),
            jax.ShapeDtypeStruct((4,) + pixel_rows.shape, jnp.bfloat16),
        ),
        in_specs=[vmem] * 5,
        out_specs=(hbm,) * 5,
        scratch_shapes=[
            pltpu.SemaphoreType.DMA((count, 19)),
            pltpu.SemaphoreType.DMA((count, 16)),
            pltpu.SemaphoreType.DMA((4, 16)),
            pltpu.SemaphoreType.DMA((4, 16)),
            pltpu.SemaphoreType.DMA((5,)),
        ],
        compiler_params=pltpu.CompilerParams(collective_id=0, has_side_effects=True),
        name="gather_all",
    )(encoder_weights, decoder_weights, border_weights, vec_tile, pixel_rows)


def pair_kernel(mine, total, got, send_sem, recv_sem):
    mate = {"tensor": 1 - lax.axis_index("tensor")}
    barrier = greet([mate])
    pl.semaphore_wait(barrier, 1)
    send(mine, got, send_sem, recv_sem, mate)
    wait_got(got, recv_sem)
    total[...] = mine[...].astype(jnp.float32) + got[...].astype(jnp.float32)
    wait_got(mine, send_sem)


def pair_total(value, which):
    low = value.astype(jnp.bfloat16)
    vmem = pl.BlockSpec(memory_space=pltpu.VMEM)
    return pl.pallas_call(
        pair_kernel,
        out_shape=jax.ShapeDtypeStruct(low.shape, jnp.float32),
        in_specs=[vmem],
        out_specs=vmem,
        scratch_shapes=[
            pltpu.VMEM(low.shape, jnp.bfloat16),
            pltpu.SemaphoreType.DMA,
            pltpu.SemaphoreType.DMA,
        ],
        compiler_params=pltpu.CompilerParams(collective_id=1 + which, has_side_effects=True),
        name="pair_total",
    )(low)


def greet_line(s):
    for k in range(1, 4):
        for sign in (-1, 1):
            other = s + sign * k
            @pl.when((other >= 0) & (other <= 3))
            def _():
                barrier = pltpu.get_barrier_semaphore()
                pl.semaphore_signal(barrier, inc=1, device_id={"seq": other}, device_id_type=MESH_ID)


def line_gather_kernel(mine, everyone, send_sem, recv_sem, own_sem):
    s = lax.axis_index("seq")
    up = {"seq": s + 1}
    down = {"seq": s - 1}
    barrier = pltpu.get_barrier_semaphore()
    for cond, device in (((s < 3), up), ((s > 0), down)):
        @pl.when(cond)
        def _():
            pl.semaphore_signal(barrier, inc=1, device_id=device, device_id_type=MESH_ID)
    pl.semaphore_wait(barrier, line_neighbours(s))
    @pl.when(s < 3)
    def _():
        send(mine, everyone.at[s], send_sem.at[0], recv_sem.at[s], up)
    @pl.when(s > 0)
    def _():
        send(mine, everyone.at[s], send_sem.at[4], recv_sem.at[s], down)
    pltpu.make_async_copy(mine, everyone.at[s], own_sem).start()
    for k in range(1, 4):
        for sign in (-1, 1):
            other = s + sign * k
            @pl.when((other >= 0) & (other <= 3))
            def _():
                place = everyone.at[other]
                wait_got(place, recv_sem.at[other])
                if k < 3 and sign < 0:
                    @pl.when(s < 3)
                    def _():
                        send(place, place, send_sem.at[k], recv_sem.at[other], up)
                if k < 3 and sign > 0:
                    @pl.when(s > 0)
                    def _():
                        send(place, place, send_sem.at[4 + k], recv_sem.at[other], down)
    for cond, slot in (
        (s < 3, 0), (s > 0, 4),
        ((s - 1 >= 0) & (s < 3), 1), ((s - 2 >= 0) & (s < 3), 2),
        ((s + 1 <= 3) & (s > 0), 5), ((s + 2 <= 3) & (s > 0), 6),
    ):
        @pl.when(cond)
        def _():
            wait_got(mine, send_sem.at[slot])
    pltpu.make_async_copy(mine, everyone.at[s], own_sem).wait()


def line_gather(rows):
    vmem = pl.BlockSpec(memory_space=pltpu.VMEM)
    return pl.pallas_call(
        line_gather_kernel,
        out_shape=jax.ShapeDtypeStruct((4,) + rows.shape, rows.dtype),
        in_specs=[vmem],
        out_specs=vmem,
        scratch_shapes=[
            pltpu.SemaphoreType.DMA((7,)),
            pltpu.SemaphoreType.DMA((4,)),
            pltpu.SemaphoreType.DMA,
        ],
        compiler_params=pltpu.CompilerParams(collective_id=12, has_side_effects=True),
        name="line_gather",
    )(rows)


def line_wait_barrier():
    barrier = pltpu.get_barrier_semaphore()
    pl.semaphore_wait(barrier, 3)


def line_reduce_kernel(parts, total, got, send_sem, recv_sem):
    s = lax.axis_index("seq")
    greet_line(s)
    line_wait_barrier()
    for k in (1, 2, 3):
        other = (s + k) % 4
        send(parts.at[other], got.at[k - 1], send_sem.at[k - 1], recv_sem.at[k - 1], {"seq": other})
    value = parts[s].astype(jnp.float32)
    for k in (1, 2, 3):
        wait_got(got.at[k - 1], recv_sem.at[k - 1])
        value = value + got[k - 1].astype(jnp.float32)
    total[...] = value
    for k in (1, 2, 3):
        wait_got(got.at[k - 1], send_sem.at[k - 1])


def line_reduce(parts, collective):
    vmem = pl.BlockSpec(memory_space=pltpu.VMEM)
    return pl.pallas_call(
        line_reduce_kernel,
        out_shape=jax.ShapeDtypeStruct(parts.shape[1:], jnp.float32),
        in_specs=[vmem],
        out_specs=vmem,
        scratch_shapes=[
            pltpu.VMEM((3,) + parts.shape[1:], parts.dtype),
            pltpu.SemaphoreType.DMA((3,)),
            pltpu.SemaphoreType.DMA((3,)),
        ],
        compiler_params=pltpu.CompilerParams(collective_id=collective, has_side_effects=True),
        name="line_reduce",
    )(parts)


def reduce_kernel(
    enc, enc_low, dec_wide, dec_low, bor, vec, loss,
    enc_o, enc_low_o, dec_wide_o, dec_low_o, bor_o, vec_o, stat_o,
    enc_r, enc_low_r, dec_wide_r, dec_low_r, bor_r, vec_r,
    line_s, line_r, vec_sum, vec_line, stat_own, stat_pair, stat_mid, stat_r, stat_mid2, stat_z,
    send_sem, recv_sem, line_send, line_recv, misc_send, misc_recv,
):
    d = lax.axis_index("dp")
    s = lax.axis_index("seq")
    t = lax.axis_index("tensor")
    rows = enc.shape[1]
    part = rows // 2
    span = dec_wide.shape[1] // 4
    small = span // 4
    mate = {"tensor": 1 - t}
    peers = (flip_low(d), flip_high(d), 3 - d)
    barrier = greet([{"dp": peer} for peer in peers] + [mate])
    greet_line(s)
    pl.semaphore_wait(barrier, 7)
    mine = pl.ds(pl.multiple_of(t * part, 8), part)

    def block(ref, dd, q):
        if q == 0:
            return ref.at[:, pl.ds(pl.multiple_of(dd * span, 8), span), :]
        return ref.at[dd]

    def bundle(dd):
        place = pl.ds(pl.multiple_of(dd * span, 8), span)
        return (
            dec_wide.at[:, place, :],
            dec_low.at[:, place, :],
            vec,
            bor.at[dd, mine, :],
            enc_low.at[:, dd],
            enc.at[dd],
        )

    lands = (dec_wide_r, dec_low_r, vec_r, bor_r, enc_low_r, enc_r)
    for item in range(6):
        for j, peer in enumerate(peers):
            send(bundle(peer)[item], lands[item].at[j], send_sem.at[item, j], recv_sem.at[item, j], {"dp": peer})

    def arrive(item):
        for j in range(3):
            wait_got(lands[item].at[j], recv_sem.at[item, j])

    own = pl.ds(pl.multiple_of(d * span, 8), span)
    arrive(0)
    arrive(1)
    wide = dec_wide[:, own, :] + dec_wide_r[0] + dec_wide_r[1] + dec_wide_r[2]
    low = dec_low[:, own, :].astype(jnp.float32)
    for j in range(3):
        low = low + dec_low_r[j].astype(jnp.float32)
    for ss in range(4):
        line_s[ss, 0:2] = wide[:, ss * small : (ss + 1) * small, :]
        line_s[ss, 2:4] = low[:, ss * small : (ss + 1) * small, :]
    arrive(2)
    vec_sum[...] = vec[...] + vec_r[0] + vec_r[1] + vec_r[2]
    for k in (1, 2, 3):
        other = (s + k) % 4
        send(line_s.at[other], line_r.at[k - 1], line_send.at[0, k - 1], line_recv.at[0, k - 1], {"seq": other})
        send(vec_sum, vec_line.at[k - 1], line_send.at[1, k - 1], line_recv.at[1, k - 1], {"seq": other})
    arrive(3)
    bor_o[mine, :] = bor[d, mine, :] + bor_r[0] + bor_r[1] + bor_r[2]
    send(bor_o.at[mine, :], bor_o.at[mine, :], misc_send.at[0], misc_recv.at[0], mate)
    bor_sum = bor[d, mine, :] + bor_r[0] + bor_r[1] + bor_r[2]
    square = jnp.sum(bor_sum * bor_sum)
    arrive(4)
    enc_sum = enc_low[:, d].astype(jnp.float32)
    for j in range(3):
        enc_sum = enc_sum + enc_low_r[j].astype(jnp.float32)
    enc_low_o[...] = enc_sum
    square = square + jnp.sum(enc_sum * enc_sum)
    arrive(5)
    enc_sum = enc[d] + enc_r[0] + enc_r[1] + enc_r[2]
    enc_o[...] = enc_sum
    square = square + jnp.sum(enc_sum * enc_sum)
    for k in (1, 2, 3):
        wait_got(line_r.at[k - 1], line_recv.at[0, k - 1])
        wait_got(vec_sum, line_recv.at[1, k - 1])
    line_sum = line_s[s] + line_r[0] + line_r[1] + line_r[2]
    dec_wide_o[...] = line_sum[0:2]
    dec_low_o[...] = line_sum[2:4]
    square = square + jnp.sum(line_sum * line_sum)
    row = lax.broadcasted_iota(jnp.int32, vec_sum.shape, 0)
    vec_all = vec_sum[...] + jnp.where(row >= 3, vec_line[0] + vec_line[1] + vec_line[2], 0.0)
    vec_o[...] = vec_all
    vec_square = jnp.sum(vec_all * vec_all)
    lane = lax.broadcasted_iota(jnp.int32, stat_own.shape, 1)
    stat_own[...] = jnp.where(lane == 2, square, loss[...])
    send(stat_own, stat_pair, misc_send.at[1], misc_recv.at[1], mate)
    wait_got(stat_pair, misc_recv.at[1])
    stat_mid[...] = stat_own[...] + stat_pair[...]
    for j, peer in enumerate(peers):
        send(stat_mid, stat_r.at[j], send_sem.at[6, j], recv_sem.at[6, j], {"dp": peer})
    for j in range(3):
        wait_got(stat_r.at[j], recv_sem.at[6, j])
    stat_mid2[...] = stat_mid[...] + stat_r[0] + stat_r[1] + stat_r[2]
    for k in (1, 2, 3):
        other = (s + k) % 4
        send(stat_mid2, stat_z.at[k - 1], line_send.at[2, k - 1], line_recv.at[2, k - 1], {"seq": other})
    for k in (1, 2, 3):
        wait_got(stat_z.at[k - 1], line_recv.at[2, k - 1])
    stat = stat_mid2[...] + stat_z[0] + stat_z[1] + stat_z[2]
    stat_o[...] = stat + jnp.where(lane == 2, vec_square, 0.0)
    for item in range(6):
        for j in range(3):
            wait_got(lands[item].at[j], send_sem.at[item, j])
    for j in range(3):
        wait_got(stat_r.at[j], send_sem.at[6, j])
        wait_got(line_r.at[j], line_send.at[0, j])
        wait_got(vec_line.at[j], line_send.at[1, j])
        wait_got(stat_z.at[j], line_send.at[2, j])
    wait_got(bor_o.at[mine, :], misc_send.at[0])
    wait_got(bor_o.at[mine, :], misc_recv.at[0])
    wait_got(stat_pair, misc_send.at[1])


def reduce_all(enc, enc_low, dec_wide, dec_low, bor, vec, loss):
    rows, width = enc.shape[1:]
    span = dec_wide.shape[1] // 4
    small = span // 4
    wide = dec_wide.shape[2]
    edge = bor.shape[2]
    vmem = pl.BlockSpec(memory_space=pltpu.VMEM)
    f32 = jnp.float32
    low = jnp.bfloat16
    stat = (8, 128)
    return pl.pallas_call(
        reduce_kernel,
        out_shape=(
            jax.ShapeDtypeStruct((rows, width), f32),
            jax.ShapeDtypeStruct((2, rows, width), f32),
            jax.ShapeDtypeStruct((2, small, wide), f32),
            jax.ShapeDtypeStruct((2, small, wide), f32),
            jax.ShapeDtypeStruct((rows, edge), f32),
            jax.ShapeDtypeStruct(vec.shape, f32),
            jax.ShapeDtypeStruct(stat, f32),
        ),
        in_specs=[vmem] * 7,
        out_specs=(vmem,) * 7,
        scratch_shapes=[
            pltpu.VMEM((3, rows, width), f32),
            pltpu.VMEM((3, 2, rows, width), low),
            pltpu.VMEM((3, 2, span, wide), f32),
            pltpu.VMEM((3, 2, span, wide), low),
            pltpu.VMEM((3, rows // 2, edge), f32),
            pltpu.VMEM((3,) + vec.shape, f32),
            pltpu.VMEM((4, 4, small, wide), f32),
            pltpu.VMEM((3, 4, small, wide), f32),
            pltpu.VMEM(vec.shape, f32),
            pltpu.VMEM((3,) + vec.shape, f32),
            pltpu.VMEM(stat, f32),
            pltpu.VMEM(stat, f32),
            pltpu.VMEM(stat, f32),
            pltpu.VMEM((3,) + stat, f32),
            pltpu.VMEM(stat, f32),
            pltpu.VMEM((3,) + stat, f32),
            pltpu.SemaphoreType.DMA((7, 3)),
            pltpu.SemaphoreType.DMA((7, 3)),
            pltpu.SemaphoreType.DMA((3, 3)),
            pltpu.SemaphoreType.DMA((3, 3)),
            pltpu.SemaphoreType.DMA((2,)),
            pltpu.SemaphoreType.DMA((2,)),
        ],
        compiler_params=pltpu.CompilerParams(collective_id=15, has_side_effects=True),
        name="reduce_all",
    )(enc, enc_low, dec_wide, dec_low, bor, vec, loss)


F32 = jnp.float32
LOW = jnp.bfloat16
SCALE = HD ** (-0.5)
ROOT_HALF = 0.5 ** 0.5
PHI_SCALE = (2.0 * math.pi) ** (-0.5)
SLAB = 4 * HD


def dot_nn(a, b):
    return lax.dot_general(a, b, (((1,), (0,)), ((), ())), preferred_element_type=F32)


def dot_nt(a, b):
    return lax.dot_general(a, b, (((1,), (1,)), ((), ())), preferred_element_type=F32)


def dot_tn(a, b):
    return lax.dot_general(a, b, (((0,), (0,)), ((), ())), preferred_element_type=F32)


def move(slab, source, target):
    rows = slab.shape[0]
    kept = slab[:, source * HD : (source + 1) * HD]
    parts = [jnp.zeros((rows, HD), slab.dtype)] * 4
    parts[target] = kept
    return jnp.concatenate(parts, axis=1)


def norm_parts(x):
    centred = x - jnp.mean(x, axis=-1, keepdims=True)
    spread = lax.rsqrt(jnp.mean(centred * centred, axis=-1, keepdims=True) + EPS_NORM)
    return centred * spread, spread


def norm_low(x, gain):
    return (norm_parts(x)[0] * gain).astype(LOW)


def norm_grads(x, gain, upstream):
    hat, spread = norm_parts(x)
    scaled = upstream * gain
    inner = jnp.mean(scaled * hat, axis=-1, keepdims=True)
    grad = spread * (scaled - jnp.mean(scaled, axis=-1, keepdims=True) - hat * inner)
    return grad, jnp.sum(upstream * hat, axis=0, keepdims=True)


def gelu_value(v):
    return 0.5 * v * (1.0 + lax.erf(v * ROOT_HALF))


def gelu_slope(v):
    return 0.5 * (1.0 + lax.erf(v * ROOT_HALF)) + v * (PHI_SCALE * jnp.exp(-0.5 * v * v))


def step_kernel(
    enc, dec, bor, gains, seen, pixels, vis_col, vis_row, table, wgt,
    enc_wide_g, enc_low_g, dec_wide_g, dec_low_g, bor_g, vec_g,
    x0, x1, x2, qkv_e, mix_e, p_e, u_e, a_e, b_e, c_e, h_e, g_e,
    z_all, a_all, qkv_d, p_d, s_d, ds_d, pl_d, mix_d, z1, z2, u_d, b_d, h_d, f_d, gp_d, g_d, pos_s, pos_c,
    lat, lat_a, lat_got, lat_b, lat_z, lat_c, enc_snd, enc_got, dec_snd, dec_got, vec_snd, vec_got,
    pair_send, pair_recv, line_send, line_recv,
):
    s = lax.axis_index("seq")
    t = lax.axis_index("tensor")
    mate = {"tensor": 1 - t}
    tubes = z1.shape[0]
    real = TUBES // 4
    seen_rows = x0.shape[0]
    own_cols = enc_low_g.shape[1]
    everyone = z_all.shape[0]
    first_core = (1 - t).astype(F32)
    barrier = greet([mate])
    greet_line(s)
    pl.semaphore_wait(barrier, 4)

    def pair_start(i, snd, got, value):
        snd[...] = value.astype(LOW)
        send(snd, got, pair_send.at[i], pair_recv.at[i], mate)

    def pair_end(i, snd, got):
        wait_got(got, pair_recv.at[i])
        return snd[...].astype(F32) + got[...].astype(F32)

    def enc_pair(i, value):
        pair_start(i, enc_snd.at[i], enc_got.at[i], value)

    def enc_sum(i):
        return pair_end(i, enc_snd.at[i], enc_got.at[i])

    def dec_pair(i, value):
        pair_start(4 + i, dec_snd.at[i], dec_got.at[i], value)

    def dec_sum(i):
        return pair_end(4 + i, dec_snd.at[i], dec_got.at[i])

    gain = [gains[i : i + 1, :] for i in range(3)]
    gain_d = [gains[i : i + 1, : z1.shape[1]] for i in range(3, 7)]
    width_d = z1.shape[1]

    angle = vis_col[...].astype(F32) * table[0:1, :]
    place = jnp.where(table[1:2, :] > 0.5, jnp.cos(angle), jnp.sin(angle))
    near_angle = lax.broadcasted_iota(jnp.int32, (tubes, width_d), 0).astype(F32) * table[2:3, :width_d]
    is_cos = table[3:4, :width_d] > 0.5
    near_sin = jnp.sin(near_angle)
    near_cos = jnp.cos(near_angle)
    pos_s[...] = jnp.where(is_cos, near_cos, near_sin)
    pos_c[...] = jnp.where(is_cos, -near_sin, near_cos)

    x0[...] = dot_nt(seen[...], bor[:, :PIX]) + place
    a_e[...] = norm_low(x0[...], gain[0])
    qkv_e[...] = dot_nn(a_e[...], enc[0]).astype(LOW)
    mix_e[...] = jnp.zeros_like(mix_e)
    enc_heads = qkv_e.shape[1] // SLAB
    key_ok = lax.broadcasted_iota(jnp.int32, (1, seen_rows), 1) < VIS

    def slab_of(h):
        return pl.ds(pl.multiple_of(h * SLAB, SLAB), SLAB)

    @pl.loop(0, enc_heads)
    def _(h):
        slab = qkv_e[:, slab_of(h)]
        scores = dot_nt(slab[:, :HD], slab[:, HD : 2 * HD]) * SCALE
        scores = jnp.where(key_ok, scores, -1e30)
        top = jnp.exp(scores - jnp.max(scores, axis=-1, keepdims=True))
        soft = top / jnp.sum(top, axis=-1, keepdims=True)
        p_e[h] = soft
        mixed = dot_nn(soft.astype(LOW), slab[:, 2 * HD : 3 * HD]).astype(LOW)
        mix_e[:, slab_of(h)] = jnp.concatenate(
            [jnp.zeros((seen_rows, 3 * HD), LOW), mixed], axis=1
        )

    enc_pair(0, dot_nt(mix_e[...], enc[0]))
    x1[...] = x0[...] + enc_sum(0)
    b_e[...] = norm_low(x1[...], gain[1])
    u_e[...] = dot_nn(b_e[...], enc[1])
    h_e[...] = gelu_value(u_e[...]).astype(LOW)
    enc_pair(1, dot_nt(h_e[...], enc[2]))
    u_e[...] = gelu_slope(u_e[...])
    x2[...] = x1[...] + enc_sum(1)
    c_e[...] = norm_low(x2[...], gain[2])
    latent = dot_nn(c_e[...], bor[:, PIX:])
    latent_high = latent.astype(LOW)
    lat[0] = latent_high
    lat[1] = (latent - latent_high.astype(F32)).astype(LOW)

    strip = 32
    strips = tubes // strip

    def strip_rows(i):
        return pl.ds(pl.multiple_of(i * strip, strip), strip)

    def block_rows(q):
        return pl.ds(pl.multiple_of(q * tubes, 32), tubes)

    def tube_column(q):
        row = lax.broadcasted_iota(jnp.int32, (tubes, 1), 0)
        return jnp.where(row < real, q * real + row, -7)

    def hidden_column(q):
        row = lax.broadcasted_iota(jnp.int32, (tubes, 1), 0)
        seen_here = (tube_column(q) == vis_row[...]).astype(F32)
        return (row < real).astype(F32) - jnp.sum(seen_here, axis=1, keepdims=True)

    @pl.loop(0, 4)
    def _(q):
        picked = tube_column(q) == vis_row[...]
        picked_low = picked.astype(F32).astype(LOW)
        hidden = hidden_column(q)
        base = (q * real).astype(F32) * table[2:3, :width_d]
        where = jnp.sin(base) * pos_c[...] + jnp.cos(base) * pos_s[...]
        z = (
            dot_nn(picked_low, lat[0])
            + dot_nn(picked_low, lat[1])
            + hidden * gain_d[3]
            + where
        )
        z_all[block_rows(q), :] = z
        normed = norm_low(z, gain_d[0])
        a_all[block_rows(q), :] = normed
        qkv_d[block_rows(q), :] = dot_nn(normed, dec[0]).astype(LOW)

    def strip_hidden(q, i):
        row = i * strip + lax.broadcasted_iota(jnp.int32, (strip, 1), 0)
        tube = jnp.where(row < real, q * real + row, -7)
        seen_here = (tube == vis_row[...]).astype(F32)
        return (row < real).astype(F32) - jnp.sum(seen_here, axis=1, keepdims=True)

    own = block_rows(s)
    dec_heads = qkv_d.shape[1] // SLAB
    mix_d[...] = jnp.zeros_like(mix_d)
    key_lane = lax.broadcasted_iota(jnp.int32, (1, everyone), 1)
    key_bias = jnp.zeros((1, everyone), F32)
    for q in range(4):
        empty = (key_lane >= q * tubes + real) & (key_lane < (q + 1) * tubes)
        key_bias = jnp.where(empty, -1e30, key_bias)

    @pl.loop(0, dec_heads)
    def _(h):
        slab = qkv_d[:, slab_of(h)]
        s_d[...] = dot_nt(move(qkv_d[own, slab_of(h)], 0, 1), slab)

        @pl.loop(0, strips)
        def _(i):
            scores = s_d[strip_rows(i), :] * SCALE + key_bias
            top = jnp.exp(scores - jnp.max(scores, axis=-1, keepdims=True))
            soft = top * (1.0 / jnp.sum(top, axis=-1, keepdims=True))
            p_d[h, strip_rows(i), :] = soft
            ds_d[strip_rows(i), :] = soft.astype(LOW)

        mix_d[:, slab_of(h)] = move(dot_nn(ds_d[...], slab).astype(LOW), 2, 3)

    dec_pair(0, dot_nt(mix_d[...], dec[0]))
    z1[...] = z_all[own, :] + dec_sum(0)
    b_d[...] = norm_low(z1[...], gain_d[1])
    u_d[...] = dot_nn(b_d[...], dec[1])

    @pl.loop(0, strips)
    def _(i):
        h_d[strip_rows(i), :] = gelu_value(u_d[strip_rows(i), :]).astype(LOW)

    dec_pair(1, dot_nt(h_d[...], dec[2]))
    z2[...] = z1[...] + dec_sum(1)
    f_d[...] = norm_low(z2[...], gain_d[2])
    share = dec.shape[2]
    wide = s_d.at[:, :share]
    wide[...] = dot_nn(f_d[...], dec[3])
    weight = wgt[0:1, 0:1]

    def head_strip(i, loss):
        target = pixels[strip_rows(i), pl.ds(pl.multiple_of(t * share, 128), share)].astype(F32)
        residue = wide[strip_rows(i), :] - target
        masked = strip_hidden(s, i) * residue
        gp_d[strip_rows(i), :] = (masked * (2.0 * weight)).astype(LOW)
        return loss + jnp.sum(masked * residue, axis=0, keepdims=True)

    loss = lax.fori_loop(0, strips, head_strip, jnp.zeros((1, share), F32))
    loss = jnp.sum(loss, axis=1, keepdims=True) * weight

    dec_pair(2, dot_nt(gp_d[...], dec[3]))
    dec_wide_g[1] = dot_tn(f_d[...], gp_d[...])
    part, gain_six = norm_grads(z2[...], gain_d[2], dec_sum(2))
    grad_z = part
    up_low = grad_z.astype(LOW)
    wide[...] = dot_nn(up_low, dec[2])

    @pl.loop(0, strips)
    def _(i):
        slope = gelu_slope(u_d[strip_rows(i), :])
        gp_d[strip_rows(i), :] = (wide[strip_rows(i), :] * slope).astype(LOW)

    dec_pair(3, dot_nt(gp_d[...], dec[1]))
    dec_low_g[1] = dot_tn(up_low, h_d[...]).astype(LOW)
    dec_low_g[0] = dot_tn(b_d[...], gp_d[...]).astype(LOW)
    part, gain_five = norm_grads(z1[...], gain_d[1], dec_sum(3))
    grad_z = grad_z + part
    z2[...] = grad_z
    up_low = grad_z.astype(LOW)
    b_d[...] = up_low
    gp_d[...] = dot_nn(up_low, dec[0]).astype(LOW)

    @pl.loop(0, dec_heads)
    def _(h):
        slab = qkv_d[:, slab_of(h)]
        grad_mix = move(gp_d[:, slab_of(h)], 3, 2)
        s_d[...] = dot_nt(grad_mix, slab)

        @pl.loop(0, strips)
        def _(i):
            soft = p_d[h, strip_rows(i), :]
            grad = s_d[strip_rows(i), :]
            ds_d[strip_rows(i), :] = (
                soft * (grad - jnp.sum(grad * soft, axis=-1, keepdims=True))
            ).astype(LOW)
            pl_d[strip_rows(i), :] = soft.astype(LOW)

        query = move(qkv_d[own, slab_of(h)], 0, 1)
        grad_query = move((dot_nn(ds_d[...], slab) * SCALE).astype(LOW), 1, 0)
        s_d[:SLAB, :] = dot_tn(query, ds_d[...]) * SCALE
        s_d[:SLAB, :] += dot_tn(grad_mix, pl_d[...])
        for q in range(4):
            g_d[q * tubes : (q + 1) * tubes, slab_of(h)] = (
                s_d[:SLAB, q * tubes : (q + 1) * tubes].T.astype(LOW)
            )
        g_d[own, slab_of(h)] = g_d[own, slab_of(h)] + grad_query

    dec_wide_g[0] = dot_tn(b_d[...], mix_d[...])
    lat_a[...] = jnp.zeros_like(lat_a)
    vec_g[...] = jnp.zeros_like(vec_g)
    lat_sum = lat_c

    def all_rows(q, carry):
        gain_four, mask_grad, latent_grad = carry
        dec_wide_g[0] += dot_tn(a_all[block_rows(q), :], g_d[block_rows(q), :])
        narrow[...] = dot_nt(g_d[block_rows(q), :], dec[0])
        share_here = jnp.where(q == s, first_core, 0.0)

        def strip_grads(i, sums):
            rows = pl.ds(pl.multiple_of(q * tubes + i * strip, strip), strip)
            part, more = norm_grads(z_all[rows, :], gain_d[0], narrow[strip_rows(i), :])
            grad = part + z2[strip_rows(i), :] * share_here
            z1[strip_rows(i), :] = grad
            masked = jnp.sum(strip_hidden(q, i) * grad, axis=0, keepdims=True)
            return (sums[0] + more, sums[1] + masked)

        gain_four, mask_grad = lax.fori_loop(0, strips, strip_grads, (gain_four, mask_grad))
        lane = lax.broadcasted_iota(jnp.int32, (1, tubes), 1)
        ids = jnp.where(lane < real, q * real + lane, -7)
        picker = (vis_col[...] == ids).astype(F32).astype(LOW)
        return (gain_four, mask_grad, latent_grad + dot_nn(picker, z1[...].astype(LOW)))

    narrow = s_d.at[:, :width_d]
    row_zero = jnp.zeros((1, width_d), F32)
    gain_four, mask_grad, latent_grad = lax.fori_loop(
        0, 4, all_rows, (row_zero, row_zero, jnp.zeros((seen_rows, width_d), F32))
    )

    lat_a[...] = latent_grad.astype(LOW)
    send(lat_a, lat_got, pair_send.at[8], pair_recv.at[8], mate)
    wait_got(lat_got, pair_recv.at[8])
    lat_b[...] = (lat_a[...].astype(F32) + lat_got[...].astype(F32)).astype(LOW)
    half = seen_rows // 2
    mine = pl.ds(pl.multiple_of(t * half, 8), half)
    for k in (1, 2, 3):
        other = (s + k) % 4
        send(lat_b.at[mine, :], lat_z.at[k - 1], line_send.at[k - 1], line_recv.at[k - 1], {"seq": other})
    total = lat_b[mine, :].astype(F32)
    for k in (1, 2, 3):
        wait_got(lat_z.at[k - 1], line_recv.at[k - 1])
        total = total + lat_z[k - 1].astype(F32)
    lat_c[mine, :] = total.astype(LOW)
    send(lat_c.at[mine, :], lat_c.at[mine, :], pair_send.at[9], pair_recv.at[9], mate)
    wait_got(lat_c.at[mine, :], pair_recv.at[9])
    wait_got(lat_c.at[mine, :], pair_send.at[9])

    grad_latent = lat_c[...]
    bor_g[:, PIX:] = dot_tn(c_e[:, :own_cols], grad_latent)
    grad_x, gain_three = norm_grads(x2[...], gain[2], dot_nt(grad_latent, bor[:, PIX:]))
    up_low = grad_x.astype(LOW)
    g_pre = (dot_nn(up_low, enc[2]) * u_e[...]).astype(LOW)
    enc_pair(2, dot_nt(g_pre, enc[1]))
    enc_low_g[1] = dot_tn(up_low[:, :own_cols], h_e[...]).astype(LOW)
    enc_low_g[0] = dot_tn(b_e[:, :own_cols], g_pre).astype(LOW)
    part, gain_two = norm_grads(x1[...], gain[1], enc_sum(2))
    grad_x = grad_x + part
    x2[...] = grad_x
    up_low = grad_x.astype(LOW)
    b_e[...] = up_low
    g_e[...] = dot_nn(up_low, enc[0]).astype(LOW)

    @pl.loop(0, enc_heads)
    def _(h):
        slab = qkv_e[:, slab_of(h)]
        grad_mix = g_e[:, slab_of(h)][:, 3 * HD :]
        soft = p_e[h]
        grad = dot_nt(grad_mix, slab[:, 2 * HD : 3 * HD])
        grad_scores = (soft * (grad - jnp.sum(grad * soft, axis=-1, keepdims=True))).astype(LOW)
        grad_query = (dot_nn(grad_scores, slab[:, HD : 2 * HD]) * SCALE).astype(LOW)
        grad_key = (dot_tn(grad_scores, slab[:, :HD]) * SCALE).astype(LOW)
        grad_value = dot_tn(soft.astype(LOW), grad_mix).astype(LOW)
        g_e[:, slab_of(h)] = jnp.concatenate(
            [grad_query, grad_key, grad_value, jnp.zeros((seen_rows, HD), LOW)], axis=1
        )

    enc_pair(3, dot_nt(g_e[...], enc[0]))
    enc_wide_g[...] = dot_tn(b_e[:, :own_cols], mix_e[...]) + dot_tn(a_e[:, :own_cols], g_e[...])
    part, gain_one = norm_grads(x0[...], gain[0], enc_sum(3))
    grad_x = x2[...] + part
    bor_g[:, :PIX] = dot_tn(grad_x[:, :own_cols].astype(LOW), seen[...])

    vec_g[0:1, :] = gain_one
    vec_g[1:2, :] = gain_two
    vec_g[2:3, :] = gain_three
    vec_g[4:5, :width_d] = gain_five
    vec_g[5:6, :width_d] = gain_six
    row = lax.broadcasted_iota(jnp.int32, vec_snd.shape, 0)
    vec_snd[...] = jnp.where(row == 3, gain_four, jnp.where(row == 6, mask_grad, 0.0))
    send(vec_snd, vec_got, pair_send.at[10], pair_recv.at[10], mate)
    wait_got(vec_got, pair_recv.at[10])
    both = vec_snd[...] + vec_got[...]
    vec_g[3:4, :width_d] = both[3:4, :]
    vec_g[6:7, :width_d] = both[6:7, :]
    vec_g[7:8, :] = jnp.broadcast_to(loss, (1, vec_g.shape[1]))
    for i in range(4):
        wait_got(enc_got.at[i], pair_send.at[i])
        wait_got(dec_got.at[i], pair_send.at[4 + i])
    wait_got(lat_got, pair_send.at[8])
    wait_got(vec_got, pair_send.at[10])
    for k in range(3):
        wait_got(lat_z.at[k], line_send.at[k])


def run_step(enc, dec, bor, gains, seen, pixels, vis_col, vis_row, table, wgt):
    v = pltpu.VMEM
    width, inner = enc.shape[1:]
    width_d, inner_d = dec.shape[1:]
    tubes = pixels.shape[0]
    everyone = 4 * tubes
    seen_rows = vis_col.shape[0]
    own_cols = width // 4
    vmem = pl.BlockSpec(memory_space=pltpu.VMEM)
    shape = jax.ShapeDtypeStruct
    return pl.pallas_call(
        step_kernel,
        out_shape=(
            shape((own_cols, inner), F32),
            shape((2, own_cols, inner), LOW),
            shape((2, width_d, inner_d), F32),
            shape((2, width_d, inner_d), LOW),
            shape((own_cols, bor.shape[1]), F32),
            shape((8, width), F32),
        ),
        in_specs=[vmem] * 10,
        out_specs=(vmem,) * 6,
        scratch_shapes=[
            v((seen_rows, width), F32), v((seen_rows, width), F32), v((seen_rows, width), F32),
            v((seen_rows, inner), LOW), v((seen_rows, inner), LOW),
            v((inner // SLAB, seen_rows, seen_rows), F32),
            v((seen_rows, inner), F32),
            v((seen_rows, width), LOW), v((seen_rows, width), LOW), v((seen_rows, width), LOW),
            v((seen_rows, inner), LOW), v((seen_rows, inner), LOW),
            v((everyone, width_d), F32), v((everyone, width_d), LOW), v((everyone, inner_d), LOW),
            v((inner_d // SLAB, tubes, everyone), F32),
            v((tubes, everyone), F32), v((tubes, everyone), LOW), v((tubes, everyone), LOW),
            v((tubes, inner_d), LOW),
            v((tubes, width_d), F32), v((tubes, width_d), F32),
            v((tubes, inner_d), F32),
            v((tubes, width_d), LOW), v((tubes, inner_d), LOW), v((tubes, width_d), LOW),
            v((tubes, inner_d), LOW),
            v((everyone, inner_d), LOW),
            v((tubes, width_d), F32), v((tubes, width_d), F32),
            v((2, seen_rows, width_d), LOW),
            v((seen_rows, width_d), LOW), v((seen_rows, width_d), LOW), v((seen_rows, width_d), LOW),
            v((3, seen_rows // 2, width_d), LOW),
            v((seen_rows, width_d), LOW),
            v((4, seen_rows, width), LOW), v((4, seen_rows, width), LOW),
            v((4, tubes, width_d), LOW), v((4, tubes, width_d), LOW),
            v((8, width_d), F32), v((8, width_d), F32),
            pltpu.SemaphoreType.DMA((11,)), pltpu.SemaphoreType.DMA((11,)),
            pltpu.SemaphoreType.DMA((3,)), pltpu.SemaphoreType.DMA((3,)),
        ],
        compiler_params=pltpu.CompilerParams(
            collective_id=1, has_side_effects=True, vmem_limit_bytes=67043328
        ),
        name="run_step",
    )(enc, dec, bor, gains, seen, pixels, vis_col, vis_row, table, wgt)


def layer_norm(x, norm_gain):
    row_mean = jnp.mean(x, axis=-1, keepdims=True)
    centred = x - row_mean
    variance = jnp.mean(centred * centred, axis=-1, keepdims=True)
    return centred * lax.rsqrt(variance + EPS_NORM) * norm_gain


def sinusoid(positions, model_width):
    half_width = model_width // 2
    frequency = jnp.exp(
        jnp.arange(half_width, dtype=jnp.float32) * (-math.log(10000.0) / half_width)
    )
    angles = positions.astype(jnp.float32)[:, None] * frequency[None, :]
    return jnp.concatenate([jnp.sin(angles), jnp.cos(angles)], axis=1)


def gelu_exact(v):
    return jax.nn.gelu(v, approximate=False)


def softmax_rows(scores):
    return jax.nn.softmax(scores, axis=-1)


def tensor_total(value):
    return lax.psum(value.astype(jnp.bfloat16), "tensor").astype(jnp.float32)


def gather_weights(encoder_weights, decoder_weights, border_weights, vector_params):
    return (
        lax.all_gather(encoder_weights, ("dp", "seq"), axis=1, tiled=True),
        lax.all_gather(decoder_weights, ("dp", "seq"), axis=1, tiled=True),
        lax.all_gather(border_weights, ("dp", "seq"), axis=0, tiled=True),
        lax.all_gather(vector_params, ("dp", "seq"), axis=0, tiled=True),
    )


def attend_forward(x, blocks, norm_gain, across):
    scale = blocks.shape[-1] ** (-0.5)
    normed, norm_back = jax.vjp(layer_norm, x, norm_gain)
    normed_low = normed.astype(jnp.bfloat16)
    projected = jnp.einsum(
        "td,dhce->chte", normed_low, blocks[:, :, :3, :], preferred_element_type=jnp.float32
    ).astype(jnp.bfloat16)
    query_rows = projected[0]
    key_rows = projected[1]
    value_rows = projected[2]
    if across:
        key_rows, value_rows = (
            lax.all_gather(key_rows, "seq", axis=1, tiled=True),
            lax.all_gather(value_rows, "seq", axis=1, tiled=True),
        )
    scores = (
        jnp.einsum("hte,hse->hts", query_rows, key_rows, preferred_element_type=jnp.float32) * scale
    )
    softmaxed, soft_back = jax.vjp(softmax_rows, scores)
    soft_low = softmaxed.astype(jnp.bfloat16)
    mixture = jnp.einsum(
        "hts,hse->hte", soft_low, value_rows, preferred_element_type=jnp.float32
    ).astype(jnp.bfloat16)
    branch = jnp.einsum(
        "hte,dhe->td", mixture, blocks[:, :, 3, :], preferred_element_type=jnp.float32
    )
    kept = (normed_low, query_rows, key_rows, value_rows, soft_low, soft_back, mixture, norm_back)
    return (x + tensor_total(branch), kept)


def attend_backward(upstream, blocks, kept, across):
    scale = blocks.shape[-1] ** (-0.5)
    normed_low, query_rows, key_rows, value_rows, soft_low, soft_back, mixture, norm_back = kept
    upstream_low = upstream.astype(jnp.bfloat16)
    grad_mixture = jnp.einsum(
        "td,dhe->hte", upstream_low, blocks[:, :, 3, :], preferred_element_type=jnp.float32
    ).astype(jnp.bfloat16)
    grad_output_w = jnp.einsum(
        "hte,td->dhe", mixture, upstream_low, preferred_element_type=jnp.float32
    )
    grad_soft = jnp.einsum(
        "hte,hse->hts", grad_mixture, value_rows, preferred_element_type=jnp.float32
    )
    grad_scores = soft_back(grad_soft)[0].astype(jnp.bfloat16)
    grad_query = (
        jnp.einsum("hts,hse->hte", grad_scores, key_rows, preferred_element_type=jnp.float32)
        * scale
    ).astype(jnp.bfloat16)
    grad_key = (
        jnp.einsum("hts,hte->hse", grad_scores, query_rows, preferred_element_type=jnp.float32)
        * scale
    )
    grad_value = jnp.einsum(
        "hts,hte->hse", soft_low, grad_mixture, preferred_element_type=jnp.float32
    )
    if across:
        grad_key, grad_value = (
            lax.psum_scatter(
                grad_key.astype(jnp.bfloat16), "seq", scatter_dimension=1, tiled=True
            ).astype(jnp.float32),
            lax.psum_scatter(
                grad_value.astype(jnp.bfloat16), "seq", scatter_dimension=1, tiled=True
            ).astype(jnp.float32),
        )
    grad_projected = jnp.stack(
        [grad_query, grad_key.astype(jnp.bfloat16), grad_value.astype(jnp.bfloat16)]
    )
    grad_input_w = jnp.einsum(
        "td,chte->dhce", normed_low, grad_projected, preferred_element_type=jnp.float32
    )
    grad_normed = tensor_total(
        jnp.einsum(
            "chte,dhce->td", grad_projected, blocks[:, :, :3, :], preferred_element_type=jnp.float32
        )
    )
    grad_x, grad_gain = norm_back(grad_normed)
    weight_grad = jnp.concatenate([grad_input_w, grad_output_w[:, :, None, :]], axis=2)
    return (upstream + grad_x, weight_grad, grad_gain)


def feed_forward_forward(x, up_proj, down_proj, norm_gain):
    normed, norm_back = jax.vjp(layer_norm, x, norm_gain)
    normed_low = normed.astype(jnp.bfloat16)
    preact = jnp.dot(normed_low, up_proj, preferred_element_type=jnp.float32)
    activation, gelu_back = jax.vjp(gelu_exact, preact)
    activation_low = activation.astype(jnp.bfloat16)
    branch = jnp.einsum("tf,df->td", activation_low, down_proj, preferred_element_type=jnp.float32)
    return (x + tensor_total(branch), (normed_low, activation_low, gelu_back, norm_back))


def feed_forward_backward(upstream, up_proj, down_proj, kept):
    normed_low, activation_low, gelu_back, norm_back = kept
    upstream_low = upstream.astype(jnp.bfloat16)
    grad_activation = jnp.dot(upstream_low, down_proj, preferred_element_type=jnp.float32)
    grad_down = jnp.einsum(
        "td,tf->df", upstream_low, activation_low, preferred_element_type=jnp.float32
    )
    grad_preact = gelu_back(grad_activation)[0].astype(jnp.bfloat16)
    grad_up = jnp.einsum("td,tf->df", normed_low, grad_preact, preferred_element_type=jnp.float32)
    grad_normed = tensor_total(
        jnp.einsum("tf,df->td", grad_preact, up_proj, preferred_element_type=jnp.float32)
    )
    grad_x, grad_gain = norm_back(grad_normed)
    return (upstream + grad_x, jnp.stack([grad_up, grad_down]), grad_gain)


def clip_step(clip_pixels, visible_row, weight, gathered):
    encoder_full, decoder_full, border_full, vector_full = gathered
    local_tubes = clip_pixels.shape[0]
    encoder_heads = encoder_full.shape[2] // (4 * HD)
    decoder_heads = decoder_full.shape[2] // (4 * HD)
    encoder_blocks = encoder_full[0].reshape(D, encoder_heads, 4, HD)
    decoder_blocks = decoder_full[0].reshape(DD, decoder_heads, 4, HD)
    vector_float = vector_full.astype(jnp.float32)
    width_ratio = D // DD
    gain_list = [
        vector_float[:, 0:width_ratio].reshape(D),
        vector_float[:, width_ratio : 2 * width_ratio].reshape(D),
        vector_float[:, 2 * width_ratio : 3 * width_ratio].reshape(D),
        vector_float[:, 3 * width_ratio],
        vector_float[:, 3 * width_ratio + 1],
        vector_float[:, 3 * width_ratio + 2],
    ]
    mask_token = vector_float[:, 3 * width_ratio + 3]
    patch_proj = border_full[:, :PIX]
    latent_proj = border_full[:, PIX:]
    pixel_head = decoder_full[3]
    tube_ids = lax.axis_index("seq") * local_tubes + jnp.arange(local_tubes, dtype=jnp.int32)
    picked = tube_ids[:, None] == visible_row[None, :]
    picked_low = picked.astype(jnp.bfloat16)
    picked_float = picked.astype(jnp.float32)
    hidden_mask = 1.0 - jnp.sum(picked_float, axis=1)
    selected = jnp.einsum("tv,tp->vp", picked_low, clip_pixels, preferred_element_type=jnp.float32)
    seen_pixels = lax.psum(selected.astype(jnp.bfloat16), "seq")
    x = jnp.einsum(
        "vp,dp->vd", seen_pixels, patch_proj, preferred_element_type=jnp.float32
    ) + sinusoid(visible_row, D)
    x, enc_attend_kept = attend_forward(x, encoder_blocks, gain_list[0], False)
    x, enc_feed_kept = feed_forward_forward(x, encoder_full[1], encoder_full[2], gain_list[1])
    encoded, encoded_back = jax.vjp(layer_norm, x, gain_list[2])
    encoded_low = encoded.astype(jnp.bfloat16)
    latent = jnp.dot(encoded_low, latent_proj, preferred_element_type=jnp.float32)
    z = (
        jnp.dot(picked_float, latent, precision=HIGH)
        + hidden_mask[:, None] * mask_token[None, :]
        + sinusoid(tube_ids, DD)
    )
    z, dec_attend_kept = attend_forward(z, decoder_blocks, gain_list[3], True)
    z, dec_feed_kept = feed_forward_forward(z, decoder_full[1], decoder_full[2], gain_list[4])
    final_norm, final_back = jax.vjp(layer_norm, z, gain_list[5])
    final_low = final_norm.astype(jnp.bfloat16)
    prediction = jnp.dot(final_low, pixel_head, preferred_element_type=jnp.float32)
    pixel_share = pixel_head.shape[1]
    target = lax.dynamic_slice_in_dim(
        clip_pixels, lax.axis_index("tensor") * pixel_share, pixel_share, 1
    ).astype(jnp.float32)
    residue = prediction - target
    loss_part = weight * jnp.sum(hidden_mask[:, None] * residue * residue)
    grad_prediction = (weight * 2.0 * hidden_mask[:, None] * residue).astype(jnp.bfloat16)
    grad_head = jnp.einsum(
        "td,tp->dp", final_low, grad_prediction, preferred_element_type=jnp.float32
    )
    grad_final = tensor_total(
        jnp.einsum("tp,dp->td", grad_prediction, pixel_head, preferred_element_type=jnp.float32)
    )
    grad_z, grad_gain_six = final_back(grad_final)
    grad_z, grad_dec_feed, grad_gain_five = feed_forward_backward(
        grad_z, decoder_full[1], decoder_full[2], dec_feed_kept
    )
    grad_z, grad_dec_attend, grad_gain_four = attend_backward(
        grad_z, decoder_blocks, dec_attend_kept, True
    )
    grad_mask = jnp.sum(hidden_mask[:, None] * grad_z, axis=0)
    latent_part = jnp.dot(picked_float.T, grad_z, precision=HIGH)
    grad_latent = lax.psum(latent_part.astype(jnp.bfloat16), "seq")
    grad_latent_proj = jnp.einsum(
        "vd,ve->de", encoded_low, grad_latent, preferred_element_type=jnp.float32
    )
    grad_encoded = jnp.einsum(
        "ve,de->vd", grad_latent, latent_proj, preferred_element_type=jnp.float32
    )
    grad_x, grad_gain_three = encoded_back(grad_encoded)
    grad_x, grad_enc_feed, grad_gain_two = feed_forward_backward(
        grad_x, encoder_full[1], encoder_full[2], enc_feed_kept
    )
    grad_x, grad_enc_attend, grad_gain_one = attend_backward(
        grad_x, encoder_blocks, enc_attend_kept, False
    )
    grad_patch = jnp.einsum(
        "vd,vp->dp", grad_x.astype(jnp.bfloat16), seen_pixels, preferred_element_type=jnp.float32
    )
    encoder_grad = jnp.stack([grad_enc_attend.reshape(D, -1), grad_enc_feed[0], grad_enc_feed[1]])
    decoder_grad = jnp.stack(
        [grad_dec_attend.reshape(DD, -1), grad_dec_feed[0], grad_dec_feed[1], grad_head]
    )
    border_grad = jnp.concatenate([grad_patch, grad_latent_proj], axis=1)
    vector_grad = jnp.concatenate(
        [
            grad_gain_one.reshape(DD, width_ratio),
            grad_gain_two.reshape(DD, width_ratio),
            grad_gain_three.reshape(DD, width_ratio),
            grad_gain_four[:, None],
            grad_gain_five[:, None],
            grad_gain_six[:, None],
            grad_mask[:, None],
        ],
        axis=1,
    )
    return (loss_part, (encoder_grad, decoder_grad, border_grad, vector_grad))


def adam_update(gradient, weights, mean_old, square_old, factor):
    scaled = gradient * factor
    mean_next = BETA_FIRST * mean_old + (1.0 - BETA_FIRST) * scaled
    square_next = BETA_SECOND * square_old + (1.0 - BETA_SECOND) * scaled * scaled
    first_fix = 1.0 - BETA_FIRST**BIAS_STEP
    second_fix = 1.0 - BETA_SECOND**BIAS_STEP
    update = -LEARN_RATE * (
        mean_next / first_fix / (jnp.sqrt(square_next / second_fix) + ADAM_EPS)
        + WEIGHT_DECAY * weights.astype(jnp.float32)
    )
    return (mean_next, square_next, update)


def local(
    pixels,
    visible,
    micro_of,
    encoder_weights,
    decoder_weights,
    border_weights,
    vector_params,
    encoder_mean,
    decoder_mean,
    border_mean,
    vector_mean,
    encoder_square,
    decoder_square,
    border_square,
    vector_square,
):
    clips_here = pixels.shape[0]
    seq_count = lax.axis_size("seq")
    dp_count = lax.axis_size("dp")
    tensor_count = lax.axis_size("tensor")
    seq_here = lax.axis_index("seq")
    micro_slots = jnp.arange(MICRO, dtype=jnp.int32)
    counts = jnp.sum((micro_of[:, None] == micro_slots[None, :]).astype(jnp.float32), axis=0)
    gathered = gather_weights(encoder_weights, decoder_weights, border_weights, vector_params)
    clip_index = lax.axis_index("dp") * clips_here + 0
    micro_index = micro_of[clip_index]
    weight = 1.0 / (counts[micro_index] * float(MICRO * (TUBES - VIS) * PIX))
    loss_part, clip_grads = clip_step(pixels[0], visible[0], weight, gathered)
    losses = loss_part * (micro_slots == micro_index).astype(jnp.float32)
    flat_count = dp_count * seq_count
    small_rows = clip_grads[3].shape[0]
    small_block = small_rows // flat_count
    small_ids = jnp.arange(small_rows, dtype=jnp.int32)
    column_ids = jnp.arange(clip_grads[3].shape[1], dtype=jnp.int32)
    small_keep = (small_ids // small_block % seq_count == seq_here).astype(jnp.float32)
    vector_keep = jnp.where(column_ids[None, :] < 3 * (D // DD), small_keep[:, None], 1.0)
    vector_total = clip_grads[3] * vector_keep
    row_ids = jnp.arange(D, dtype=jnp.int32)
    row_keep = (row_ids // (D // flat_count) % seq_count == seq_here).astype(jnp.float32)
    summed = (
        lax.psum_scatter(
            clip_grads[0] * row_keep[None, :, None], ("dp", "seq"), scatter_dimension=1, tiled=True
        ),
        lax.psum_scatter(clip_grads[1], ("dp", "seq"), scatter_dimension=1, tiled=True),
        lax.psum_scatter(
            clip_grads[2] * row_keep[:, None], ("dp", "seq"), scatter_dimension=0, tiled=True
        ),
        lax.psum_scatter(vector_total, ("dp", "seq"), scatter_dimension=0, tiled=True),
    )
    square_sum = (
        jnp.sum(summed[0] * summed[0])
        + jnp.sum(summed[1] * summed[1])
        + (jnp.sum(summed[2] * summed[2]) + jnp.sum(summed[3] * summed[3])) / tensor_count
    )
    losses_all, square_all = lax.psum((losses, square_sum), ("dp", "seq", "tensor"))
    grad_norm = jnp.sqrt(square_all)
    factor = jnp.minimum(1.0, CLIP_LIMIT / grad_norm)
    enc_next = adam_update(summed[0], encoder_weights, encoder_mean, encoder_square, factor)
    dec_next = adam_update(summed[1], decoder_weights, decoder_mean, decoder_square, factor)
    bor_next = adam_update(summed[2], border_weights, border_mean, border_square, factor)
    vec_next = adam_update(summed[3], vector_params, vector_mean, vector_square, factor)
    return (
        enc_next[0],
        enc_next[1],
        enc_next[2],
        dec_next[0],
        dec_next[1],
        dec_next[2],
        bor_next[0],
        bor_next[1],
        bor_next[2],
        vec_next[0],
        vec_next[1],
        vec_next[2],
        losses_all,
        jnp.reshape(grad_norm, (1,)),
    )


def fits_fast(mesh):
    return dict(mesh.shape) == {"dp": 4, "seq": 4, "tensor": 2}


def turned(values, s, rows):
    blocks = values.reshape((4, 4, rows) + values.shape[1:])
    return jnp.swapaxes(jnp.roll(blocks, -s, axis=1), 0, 1).reshape(values.shape)


def fast_local(
    pixels,
    visible,
    micro_of,
    encoder_weights,
    decoder_weights,
    border_weights,
    vector_params,
    encoder_mean,
    decoder_mean,
    border_mean,
    vector_mean,
    encoder_square,
    decoder_square,
    border_square,
    vector_square,
):
    low = jnp.bfloat16
    clip_pixels = pixels[0]
    visible_row = visible[0]
    s = lax.axis_index("seq")
    rows = encoder_weights.shape[1]
    small = decoder_weights.shape[1]
    own = 4 * rows
    micro_slots = jnp.arange(MICRO, dtype=jnp.int32)
    counts = jnp.sum((micro_of[:, None] == micro_slots[None, :]).astype(jnp.float32), axis=0)
    micro_index = micro_of[lax.axis_index("dp")]
    weight = 1.0 / (counts[micro_index] * float(MICRO * (TUBES - VIS) * PIX))
    local_tubes = clip_pixels.shape[0]
    tube_ids = s * local_tubes + jnp.arange(local_tubes, dtype=jnp.int32)
    picked = tube_ids[:, None] == visible_row[None, :]
    picked_float = picked.astype(jnp.float32)
    hidden_mask = 1.0 - jnp.sum(picked_float, axis=1)
    selected = jnp.einsum(
        "tv,tp->vp", picked.astype(low), clip_pixels, preferred_element_type=jnp.float32
    ).astype(low)
    own_vectors = vector_params.astype(jnp.float32)
    ratio = D // DD
    lines = [own_vectors[:, ratio * i : ratio * (i + 1)].reshape(1, rows) for i in range(3)]
    lines += [
        jnp.pad(own_vectors[:, 3 * ratio + i].reshape(1, small), ((0, 0), (0, rows - small)))
        for i in range(4)
    ]
    tile = jnp.pad(jnp.concatenate(lines), ((0, 1), (0, 128 - rows)))
    encoder_full, decoder_full, border_full, vector_tiles, pixel_parts = gather_all(
        encoder_weights, decoder_weights, border_weights, tile, jnp.pad(selected, ((0, 3), (0, 0)))
    )
    gains = [turned(vector_tiles[:, i, :rows].reshape(D), s, rows) for i in range(3)]
    gains += [vector_tiles[:, 3 + i, :small].reshape(DD) for i in range(4)]
    rows_of = [g[None, :] for g in gains[:3]] + [
        jnp.pad(g, (0, D - DD))[None, :] for g in gains[3:]
    ]
    gain_rows = jnp.pad(jnp.concatenate(rows_of), ((0, 1), (0, 0)))
    column = turned(jnp.arange(D, dtype=jnp.int32), s, rows)
    half_d, half_dd = D // 2, DD // 2
    column_d = jnp.arange(D, dtype=jnp.int32)
    table = jnp.stack(
        [
            jnp.exp((column % half_d).astype(jnp.float32) * (-math.log(10000.0) / half_d)),
            (column >= half_d).astype(jnp.float32),
            jnp.exp((column_d % half_dd).astype(jnp.float32) * (-math.log(10000.0) / half_dd)),
            (column_d >= half_dd).astype(jnp.float32),
        ]
    )
    table = jnp.pad(table, ((0, 4), (0, 0)))
    padded = jnp.pad(visible_row, (0, 3), constant_values=-1)
    enc_wide, enc_low, dec_wide, dec_low, border_grad, vector_rows = run_step(
        encoder_full,
        decoder_full,
        border_full,
        gain_rows,
        jnp.sum(pixel_parts.astype(jnp.float32), axis=0).astype(low),
        jnp.pad(clip_pixels, ((0, -local_tubes % 32), (0, 0))),
        padded[:, None],
        padded[None, :],
        table,
        jnp.full((8, 128), weight, jnp.float32),
    )
    loss_part = vector_rows[7, 0]
    vector_rows = vector_rows * (jnp.arange(8)[:, None] < 7).astype(jnp.float32)
    losses = loss_part * (micro_slots == micro_index).astype(jnp.float32)
    loss_tile = jnp.pad(losses[None, :], ((0, 7), (0, 126)))
    enc_wide_sum, enc_low_sum, wide_sum, low_sum, border_sum, vector_sum, stats = reduce_all(
        enc_wide.reshape(4, rows, -1),
        enc_low.reshape(2, 4, rows, -1),
        dec_wide,
        dec_low,
        border_grad.reshape(4, rows, -1),
        vector_rows,
        loss_tile,
    )
    enc_sum = jnp.concatenate([enc_wide_sum[None], enc_low_sum])
    dec_sum = jnp.stack([wide_sum[0], low_sum[0], low_sum[1], wide_sum[1]])
    d = lax.axis_index("dp")
    first_rows = lax.dynamic_slice(vector_sum, (0, d * rows), (3, rows))
    later_rows = lax.dynamic_slice(vector_sum, (3, (d * 4 + s) * small), (4, small))
    vector_own = jnp.concatenate(
        [first_rows[i].reshape(small, ratio) for i in range(3)] + [later_rows.T], axis=1
    )
    grad_norm = jnp.sqrt(stats[0, 2])
    factor = jnp.minimum(1.0, CLIP_LIMIT / grad_norm)
    enc_next = adam_update(enc_sum, encoder_weights, encoder_mean, encoder_square, factor)
    dec_next = adam_update(dec_sum, decoder_weights, decoder_mean, decoder_square, factor)
    bor_next = adam_update(border_sum, border_weights, border_mean, border_square, factor)
    vec_next = adam_update(vector_own, vector_params, vector_mean, vector_square, factor)
    return (
        *enc_next,
        *dec_next,
        *bor_next,
        *vec_next,
        stats[0, :MICRO],
        jnp.reshape(grad_norm, (1,)),
    )


def solution(mesh):
    in_specs = (
        P("dp", "seq", None),
        P("dp", None),
        P(),
        P(None, ("dp", "seq"), "tensor"),
        P(None, ("dp", "seq"), "tensor"),
        P(("dp", "seq"), None),
        P(("dp", "seq"), None),
        P(None, ("dp", "seq"), "tensor"),
        P(None, ("dp", "seq"), "tensor"),
        P(("dp", "seq"), None),
        P(("dp", "seq"), None),
        P(None, ("dp", "seq"), "tensor"),
        P(None, ("dp", "seq"), "tensor"),
        P(("dp", "seq"), None),
        P(("dp", "seq"), None),
    )
    out_specs = (
        P(None, ("dp", "seq"), "tensor"),
        P(None, ("dp", "seq"), "tensor"),
        P(None, ("dp", "seq"), "tensor"),
        P(None, ("dp", "seq"), "tensor"),
        P(None, ("dp", "seq"), "tensor"),
        P(None, ("dp", "seq"), "tensor"),
        P(("dp", "seq"), None),
        P(("dp", "seq"), None),
        P(("dp", "seq"), None),
        P(("dp", "seq"), None),
        P(("dp", "seq"), None),
        P(("dp", "seq"), None),
        P(),
        P(),
    )
    chosen = fast_local if fits_fast(mesh) else local
    return jax.shard_map(chosen, mesh=mesh, in_specs=in_specs, out_specs=out_specs, check_vma=False)
```

```python
import math

import jax
import jax.numpy as jnp
from jax import lax
from jax.experimental import pallas as pl
from jax.experimental.pallas import tpu as pltpu
from jax.sharding import PartitionSpec as P

PIX = 1536
D = 768
HD = 64
DD = 384
TUBES = 1568
VIS = 157
MICRO = 2


HIGH = lax.Precision.HIGHEST
EPS_NORM = 1e-06
CLIP_LIMIT = 0.025
LEARN_RATE = 0.01
WEIGHT_DECAY = 0.05
BETA_FIRST = 0.9
BETA_SECOND = 0.999
ADAM_EPS = 1e-08
BIAS_STEP = 10.0


MESH_ID = pl.DeviceIdType.MESH


def flip_low(d):
    return d + 1 - 2 * (d % 2)


def flip_high(d):
    return (d + 2) % 4


def line_neighbours(s):
    return 1 - s // 3 + (s + 2) // 3


def send(source, target, send_sem, recv_sem, device):
    copy = pltpu.make_async_remote_copy(
        src_ref=source,
        dst_ref=target,
        send_sem=send_sem,
        recv_sem=recv_sem,
        device_id=device,
        device_id_type=MESH_ID,
    )
    copy.start()


def wait_got(place, recv_sem):
    pltpu.make_async_copy(place, place, recv_sem).wait()


def greet(devices):
    barrier = pltpu.get_barrier_semaphore()
    for device in devices:
        pl.semaphore_signal(barrier, inc=1, device_id=device, device_id_type=MESH_ID)
    return barrier


def gather_kernel(enc, dec, bor, vec, pix, enc_o, dec_o, bor_o, vec_o, pix_o, send_sem, recv_sem, pair_send, pair_recv, own_sem):
    d = lax.axis_index("dp")
    s = lax.axis_index("seq")
    t = lax.axis_index("tensor")
    rows = enc.shape[1]
    small = dec.shape[1]
    part = rows // 2
    near = {"dp": flip_low(d)}
    far = {"dp": flip_high(d)}
    up = {"seq": s + 1}
    down = {"seq": s - 1}
    mate = {"tensor": 1 - t}
    d_near = flip_low(d)
    d_far = flip_high(d)
    d_diag = 3 - d

    def enc_place(m, c0, w):
        def at(viewer, dd, ss):
            slot = ((ss - viewer + 4) % 4) * 4 + dd
            return enc_o.at[m, pl.ds(pl.multiple_of(slot * rows, 8), rows), c0 : c0 + w]
        return (enc.at[m, :, c0 : c0 + w], at)

    def bor_place(c0, w):
        def at(viewer, dd, ss):
            slot = ((ss - viewer + 4) % 4) * 4 + dd
            return bor_o.at[pl.ds(pl.multiple_of(slot * rows + t * part, 8), part), c0 : c0 + w]
        return (bor.at[pl.ds(pl.multiple_of(t * part, 8), part), c0 : c0 + w], at)

    def dec_place(m):
        def at(viewer, dd, ss):
            return dec_o.at[m, pl.ds(pl.multiple_of((dd * 4 + ss) * small, 8), small), :]
        return (dec.at[m], at)

    def vec_place():
        def at(viewer, dd, ss):
            return vec_o.at[dd * 4 + ss]
        return (vec, at)

    def pix_place():
        half = pix.shape[1] // 2
        cols = pl.ds(pl.multiple_of(t * half, 128), half)
        def at(viewer, dd, ss):
            return pix_o.at[ss, :, cols]
        return (pix.at[:, cols], at)

    pieces = [
        (0, False, vec_place()),
        (2, True, pix_place()),
        (0, True, bor_place(0, 768)),
        (1, True, bor_place(768, 768)),
        (0, False, enc_place(0, 0, 768)),
        (1, False, enc_place(0, 768, 768)),
        (0, False, enc_place(1, 0, 768)),
        (1, False, enc_place(1, 768, 768)),
        (0, False, enc_place(2, 0, 768)),
        (1, False, enc_place(2, 768, 768)),
        (0, True, bor_place(1536, 384)),
        (1, False, dec_place(0)),
        (0, False, dec_place(1)),
        (1, False, dec_place(2)),
        (0, False, dec_place(3)),
    ]
    paired = [p for p in range(len(pieces)) if pieces[p][1]]

    barrier = greet([near, far, mate])
    @pl.when(s < 3)
    def _():
        pl.semaphore_signal(barrier, inc=1, device_id=up, device_id_type=MESH_ID)
    @pl.when(s > 0)
    def _():
        pl.semaphore_signal(barrier, inc=1, device_id=down, device_id_type=MESH_ID)
    pl.semaphore_wait(barrier, 3 + line_neighbours(s))

    def hops(kind):
        return (near, far) if kind == 0 else (far, near)

    for p, (kind, pair, (own, at)) in enumerate(pieces):
        got = recv_sem.at[p, d * 4 + s]
        @pl.when(s < 3)
        def _():
            send(own, at(s + 1, d, s), send_sem.at[p, 0], got, up)
        @pl.when(s > 0)
        def _():
            send(own, at(s - 1, d, s), send_sem.at[p, 4], got, down)
        if kind != 2:
            first, second = hops(kind)
            send(own, at(s, d, s), send_sem.at[p, 5], got, first)
            send(own, at(s, d, s), send_sem.at[p, 9], got, second)
    own_copies = [
        (enc, enc_o.at[:, pl.ds(pl.multiple_of(d * rows, 8), rows), :]),
        (dec, dec_o.at[:, pl.ds(pl.multiple_of((d * 4 + s) * small, 8), small), :]),
        (bor, bor_o.at[pl.ds(pl.multiple_of(d * rows, 8), rows), :]),
        (vec, vec_o.at[d * 4 + s]),
        (pix, pix_o.at[s]),
    ]
    for j, (source, target) in enumerate(own_copies):
        pltpu.make_async_copy(source, target, own_sem.at[j]).start()

    def to_mate(p, at, dd, ss):
        if pieces[p][1]:
            q = paired.index(p)
            place = at(s, dd, ss)
            send(place, place, pair_send.at[q, dd * 4 + ss], pair_recv.at[q, dd * 4 + ss], mate)

    def column(p):
        kind, pair, (own, at) = pieces[p]
        for k in range(1, 4):
            for sign in (-1, 1):
                ss = s + sign * k
                @pl.when((ss >= 0) & (ss <= 3))
                def _():
                    place = at(s, d, ss)
                    got = recv_sem.at[p, d * 4 + ss]
                    wait_got(place, got)
                    if k < 3:
                        if sign < 0:
                            @pl.when(s < 3)
                            def _():
                                send(place, at(s + 1, d, ss), send_sem.at[p, k], got, up)
                        else:
                            @pl.when(s > 0)
                            def _():
                                send(place, at(s - 1, d, ss), send_sem.at[p, 16 + k], got, down)
                    if kind != 2:
                        first, second = hops(kind)
                        send(place, place, send_sem.at[p, 5 + (ss - s + 4) % 4], got, first)
                        send(place, place, send_sem.at[p, 9 + (ss - s + 4) % 4], got, second)
                    to_mate(p, at, d, ss)

    def plane(p):
        kind, pair, (own, at) = pieces[p]
        if kind == 2:
            return
        dd = d_near if kind == 0 else d_far
        second = hops(kind)[1]
        for k in range(0, 4):
            for sign in (-1, 1) if k else (1,):
                ss = s + sign * k
                @pl.when((ss >= 0) & (ss <= 3))
                def _():
                    place = at(s, dd, ss)
                    got = recv_sem.at[p, dd * 4 + ss]
                    wait_got(place, got)
                    send(place, place, send_sem.at[p, 13 + (ss - s + 4) % 4], got, second)
                    to_mate(p, at, dd, ss)

    def last(p):
        kind, pair, (own, at) = pieces[p]
        if kind == 2:
            return
        for dd in (d_far, d_diag) if kind == 0 else (d_near, d_diag):
            for k in range(0, 4):
                for sign in (-1, 1) if k else (1,):
                    ss = s + sign * k
                    @pl.when((ss >= 0) & (ss <= 3))
                    def _():
                        place = at(s, dd, ss)
                        wait_got(place, recv_sem.at[p, dd * 4 + ss])
                        to_mate(p, at, dd, ss)

    def drain(p):
        kind, pair, (own, at) = pieces[p]
        def sent(slot):
            wait_got(own, send_sem.at[p, slot])
        @pl.when(s < 3)
        def _():
            sent(0)
        @pl.when(s > 0)
        def _():
            sent(4)
        for k in (1, 2):
            @pl.when((s - k >= 0) & (s < 3))
            def _():
                sent(k)
            @pl.when((s + k <= 3) & (s > 0))
            def _():
                sent(16 + k)
        if kind != 2:
            for slot in range(5, 17):
                sent(slot)
        if pair:
            q = paired.index(p)
            t_other = 1 - t
            for dd in (d, d_near, d_far, d_diag):
                for ss_rel in range(4):
                    ss = (s + ss_rel) % 4
                    if ss_rel == 0 and dd is d:
                        continue
                    if kind == 2 and dd is not d:
                        continue
                    wait_got(own, pair_send.at[q, dd * 4 + ss])
                    wait_got(own, pair_recv.at[q, dd * 4 + ss])

    count = len(pieces)
    for p in range(count):
        column(p)
        if p >= 1:
            plane(p - 1)
        if p >= 3:
            last(p - 3)
    plane(count - 1)
    for p in range(count - 3, count):
        last(p)
    for p in range(count):
        drain(p)
    for j, (source, target) in enumerate(own_copies):
        pltpu.make_async_copy(source, target, own_sem.at[j]).wait()


def gather_all(encoder_weights, decoder_weights, border_weights, vec_tile, pixel_rows):
    rows = encoder_weights.shape[1]
    small = decoder_weights.shape[1]
    hbm = pl.BlockSpec(memory_space=pl.ANY)
    vmem = pl.BlockSpec(memory_space=pltpu.VMEM)
    count = 15
    return pl.pallas_call(
        gather_kernel,
        out_shape=(
            jax.ShapeDtypeStruct((3, rows * 16, encoder_weights.shape[2]), jnp.bfloat16),
            jax.ShapeDtypeStruct((4, small * 16, decoder_weights.shape[2]), jnp.bfloat16),
            jax.ShapeDtypeStruct((rows * 16, border_weights.shape[1]), jnp.bfloat16),
            jax.ShapeDtypeStruct((16,) + vec_tile.shape, jnp.float32),
            jax.ShapeDtypeStruct((4,) + pixel_rows.shape, jnp.bfloat16),
        ),
        in_specs=[vmem] * 5,
        out_specs=(hbm,) * 5,
        scratch_shapes=[
            pltpu.SemaphoreType.DMA((count, 19)),
            pltpu.SemaphoreType.DMA((count, 16)),
            pltpu.SemaphoreType.DMA((4, 16)),
            pltpu.SemaphoreType.DMA((4, 16)),
            pltpu.SemaphoreType.DMA((5,)),
        ],
        compiler_params=pltpu.CompilerParams(collective_id=0, has_side_effects=True),
        name="gather_all",
    )(encoder_weights, decoder_weights, border_weights, vec_tile, pixel_rows)


def greet_line(s):
    for k in range(1, 4):
        for sign in (-1, 1):
            other = s + sign * k
            @pl.when((other >= 0) & (other <= 3))
            def _():
                barrier = pltpu.get_barrier_semaphore()
                pl.semaphore_signal(barrier, inc=1, device_id={"seq": other}, device_id_type=MESH_ID)


F32 = jnp.float32
LOW = jnp.bfloat16
SCALE = HD ** (-0.5)
ROOT_HALF = 0.5 ** 0.5
PHI_SCALE = (2.0 * math.pi) ** (-0.5)
SLAB = 4 * HD


def dot_nn(a, b):
    return lax.dot_general(a, b, (((1,), (0,)), ((), ())), preferred_element_type=F32)


def dot_nt(a, b):
    return lax.dot_general(a, b, (((1,), (1,)), ((), ())), preferred_element_type=F32)


def dot_tn(a, b):
    return lax.dot_general(a, b, (((0,), (0,)), ((), ())), preferred_element_type=F32)


def move(slab, source, target):
    rows = slab.shape[0]
    kept = slab[:, source * HD : (source + 1) * HD]
    parts = [jnp.zeros((rows, HD), slab.dtype)] * 4
    parts[target] = kept
    return jnp.concatenate(parts, axis=1)


def norm_parts(x):
    centred = x - jnp.mean(x, axis=-1, keepdims=True)
    spread = lax.rsqrt(jnp.mean(centred * centred, axis=-1, keepdims=True) + EPS_NORM)
    return centred * spread, spread


def norm_low(x, gain):
    return (norm_parts(x)[0] * gain).astype(LOW)


def norm_grads(x, gain, upstream):
    hat, spread = norm_parts(x)
    scaled = upstream * gain
    inner = jnp.mean(scaled * hat, axis=-1, keepdims=True)
    grad = spread * (scaled - jnp.mean(scaled, axis=-1, keepdims=True) - hat * inner)
    return grad, jnp.sum(upstream * hat, axis=0, keepdims=True)


def gelu_value(v):
    return 0.5 * v * (1.0 + lax.erf(v * ROOT_HALF))


def gelu_slope(v):
    return 0.5 * (1.0 + lax.erf(v * ROOT_HALF)) + v * (PHI_SCALE * jnp.exp(-0.5 * v * v))


def step_kernel(
    enc, dec, bor, gains, seen, pixels, vis_col, vis_row, table, wgt, micro,
    enc_wide_o, enc_low_o, attend_o, low_o, head_o, bor_o, vec_o, stat_o,
    x0, x1, x2, qkv_e, mix_e, p_e, u_e, a_e, b_e, c_e, h_e,
    z_all, a_all, qkv_d, p_d, s_d, ds_d, mix_d, z1, z2, u_d, b_d, h_d, f_d, gp_d, g_d, pos_s, pos_c,
    lat, lat_a, lat_got, lat_b, lat_z, lat_c, enc_snd, enc_got, dec_snd, dec_got, vec_g, vec_got,
    enc_wide_g, enc_low_g, attend_g, low_g, head_g, bor_g,
    enc_wide_r, enc_low_r, attend_r, low_r, head_r, bor_r, vec_r,
    head_z, head_zr, attend_z, attend_zr, low_z, low_zr, vec_z, vec_zr, vec_p, stat, stat_r,
    pair_send, pair_recv, line_send, line_recv, plane_send, plane_recv,
):
    s = lax.axis_index("seq")
    t = lax.axis_index("tensor")
    mate = {"tensor": 1 - t}
    tubes = z1.shape[0]
    real = TUBES // 4
    seen_rows = x0.shape[0]
    rows = enc_wide_g.shape[1]
    own_cols = 4 * rows
    part_rows = rows // 2
    everyone = z_all.shape[0]
    first_core = (1 - t).astype(F32)
    d = lax.axis_index("dp")
    peers = (flip_low(d), flip_high(d), 3 - d)
    barrier = greet([{"dp": peer} for peer in peers] + [mate])
    greet_line(s)
    pl.semaphore_wait(barrier, 7)

    def to_plane(item, piece, landing):
        for j, peer in enumerate(peers):
            send(piece(peer), landing.at[j], plane_send.at[item, j], plane_recv.at[item, j], {"dp": peer})

    def plane_total(item, own_value, landing):
        total = own_value
        for j in range(3):
            wait_got(landing.at[j], plane_recv.at[item, j])
            total = total + landing[j].astype(F32)
        return total

    def to_line(item, piece, landing):
        for k in (1, 2, 3):
            other = (s + k) % 4
            send(piece(other), landing.at[k - 1], line_send.at[item, k - 1], line_recv.at[item, k - 1], {"seq": other})

    def line_total(item, own_value, landing):
        total = own_value
        for k in range(3):
            wait_got(landing.at[k], line_recv.at[item, k])
            total = total + landing[k].astype(F32)
        return total

    def pair_start(i, snd, got, value, before=None):
        if before is not None:
            wait_got(snd, pair_send.at[before])
        snd[...] = value.astype(LOW)
        send(snd, got, pair_send.at[i], pair_recv.at[i], mate)

    def pair_end(i, snd, got):
        wait_got(got, pair_recv.at[i])
        return snd[...].astype(F32) + got[...].astype(F32)

    def enc_pair(i, value):
        pair_start(i, enc_snd.at[i % 2], enc_got.at[i % 2], value, i - 2 if i >= 2 else None)

    def enc_sum(i):
        return pair_end(i, enc_snd.at[i % 2], enc_got.at[i % 2])

    def dec_pair(i, value):
        pair_start(4 + i, dec_snd.at[i % 2], dec_got.at[i % 2], value, 2 + i if i >= 2 else None)

    def dec_sum(i):
        return pair_end(4 + i, dec_snd.at[i % 2], dec_got.at[i % 2])

    gain = [gains[i : i + 1, :] for i in range(3)]
    gain_d = [gains[i : i + 1, : z1.shape[1]] for i in range(3, 7)]
    width_d = z1.shape[1]

    angle = vis_col[...].astype(F32) * table[0:1, :]
    place = jnp.where(table[1:2, :] > 0.5, jnp.cos(angle), jnp.sin(angle))
    near_angle = lax.broadcasted_iota(jnp.int32, (tubes, width_d), 0).astype(F32) * table[2:3, :width_d]
    is_cos = table[3:4, :width_d] > 0.5
    near_sin = jnp.sin(near_angle)
    near_cos = jnp.cos(near_angle)
    pos_s[...] = jnp.where(is_cos, near_cos, near_sin)
    pos_c[...] = jnp.where(is_cos, -near_sin, near_cos)

    x0[...] = dot_nt(seen[...], bor[:, :PIX]) + place
    a_e[...] = norm_low(x0[...], gain[0])
    qkv_e[...] = dot_nn(a_e[...], enc[0]).astype(LOW)
    mix_e[...] = jnp.zeros_like(mix_e)
    enc_heads = qkv_e.shape[1] // SLAB
    key_ok = lax.broadcasted_iota(jnp.int32, (1, seen_rows), 1) < VIS

    def slab_of(h):
        return pl.ds(pl.multiple_of(h * SLAB, SLAB), SLAB)

    @pl.loop(0, enc_heads)
    def _(h):
        slab = qkv_e[:, slab_of(h)]
        scores = dot_nt(slab[:, :HD], slab[:, HD : 2 * HD]) * SCALE
        scores = jnp.where(key_ok, scores, -1e30)
        top = jnp.exp(scores - jnp.max(scores, axis=-1, keepdims=True))
        soft = top / jnp.sum(top, axis=-1, keepdims=True)
        p_e[h] = soft.astype(LOW)
        mixed = dot_nn(soft.astype(LOW), slab[:, 2 * HD : 3 * HD]).astype(LOW)
        mix_e[:, slab_of(h)] = jnp.concatenate(
            [jnp.zeros((seen_rows, 3 * HD), LOW), mixed], axis=1
        )

    enc_pair(0, dot_nt(mix_e[...], enc[0]))
    x1[...] = x0[...] + enc_sum(0)
    b_e[...] = norm_low(x1[...], gain[1])
    u_e[...] = dot_nn(b_e[...], enc[1])
    h_e[...] = gelu_value(u_e[...]).astype(LOW)
    enc_pair(1, dot_nt(h_e[...], enc[2]))
    u_e[...] = gelu_slope(u_e[...])
    x2[...] = x1[...] + enc_sum(1)
    c_e[...] = norm_low(x2[...], gain[2])
    latent = dot_nn(c_e[...], bor[:, PIX:])
    latent_high = latent.astype(LOW)
    lat[0] = latent_high
    lat[1] = (latent - latent_high.astype(F32)).astype(LOW)

    strip = 32
    strips = tubes // strip

    def strip_rows(i):
        return pl.ds(pl.multiple_of(i * strip, strip), strip)

    def block_rows(q):
        return pl.ds(pl.multiple_of(q * tubes, 32), tubes)

    def tube_column(q):
        row = lax.broadcasted_iota(jnp.int32, (tubes, 1), 0)
        return jnp.where(row < real, q * real + row, -7)

    def hidden_column(q):
        row = lax.broadcasted_iota(jnp.int32, (tubes, 1), 0)
        seen_here = (tube_column(q) == vis_row[...]).astype(F32)
        return (row < real).astype(F32) - jnp.sum(seen_here, axis=1, keepdims=True)

    @pl.loop(0, 4)
    def _(q):
        picked = tube_column(q) == vis_row[...]
        picked_low = picked.astype(F32).astype(LOW)
        hidden = hidden_column(q)
        base = (q * real).astype(F32) * table[2:3, :width_d]
        where = jnp.sin(base) * pos_c[...] + jnp.cos(base) * pos_s[...]
        z = (
            dot_nn(picked_low, lat[0])
            + dot_nn(picked_low, lat[1])
            + hidden * gain_d[3]
            + where
        )
        z_all[block_rows(q), :] = z
        normed = norm_low(z, gain_d[0])
        a_all[block_rows(q), :] = normed
        qkv_d[block_rows(q), :] = dot_nn(normed, dec[0]).astype(LOW)

    def strip_hidden(q, i):
        row = i * strip + lax.broadcasted_iota(jnp.int32, (strip, 1), 0)
        tube = jnp.where(row < real, q * real + row, -7)
        seen_here = (tube == vis_row[...]).astype(F32)
        return (row < real).astype(F32) - jnp.sum(seen_here, axis=1, keepdims=True)

    own = block_rows(s)
    dec_heads = qkv_d.shape[1] // SLAB
    mix_d[...] = jnp.zeros_like(mix_d)
    key_lane = lax.broadcasted_iota(jnp.int32, (1, everyone), 1)
    key_bias = jnp.zeros((1, everyone), F32)
    for q in range(4):
        empty = (key_lane >= q * tubes + real) & (key_lane < (q + 1) * tubes)
        key_bias = jnp.where(empty, -1e30, key_bias)

    @pl.loop(0, dec_heads)
    def _(h):
        slab = qkv_d[:, slab_of(h)]
        s_d[...] = dot_nt(move(qkv_d[own, slab_of(h)], 0, 1), slab)

        @pl.loop(0, strips)
        def _(i):
            scores = s_d[strip_rows(i), :] * SCALE + key_bias
            top = jnp.exp(scores - jnp.max(scores, axis=-1, keepdims=True))
            soft = top * (1.0 / jnp.sum(top, axis=-1, keepdims=True))
            p_d[h, strip_rows(i), :] = soft.astype(LOW)

        mix_d[:, slab_of(h)] = move(dot_nn(p_d[h], slab).astype(LOW), 2, 3)

    dec_pair(0, dot_nt(mix_d[...], dec[0]))
    z1[...] = z_all[own, :] + dec_sum(0)
    b_d[...] = norm_low(z1[...], gain_d[1])
    u_d[...] = dot_nn(b_d[...], dec[1])

    @pl.loop(0, strips)
    def _(i):
        h_d[strip_rows(i), :] = gelu_value(u_d[strip_rows(i), :]).astype(LOW)

    dec_pair(1, dot_nt(h_d[...], dec[2]))
    z2[...] = z1[...] + dec_sum(1)
    f_d[...] = norm_low(z2[...], gain_d[2])
    share = dec.shape[2]
    wide = s_d.at[:, :share]
    wide[...] = dot_nn(f_d[...], dec[3])
    weight = wgt[0:1, 0:1]

    def head_strip(i, loss):
        target = pixels[strip_rows(i), :].astype(F32)
        residue = wide[strip_rows(i), :] - target
        masked = strip_hidden(s, i) * residue
        gp_d[strip_rows(i), :] = (masked * (2.0 * weight)).astype(LOW)
        return loss + jnp.sum(masked * residue, axis=0, keepdims=True)

    loss = lax.fori_loop(0, strips, head_strip, jnp.zeros((1, share), F32))
    loss = jnp.sum(loss, axis=1, keepdims=True) * weight

    dec_pair(2, dot_nt(gp_d[...], dec[3]))
    head_g[...] = dot_tn(f_d[...], gp_d[...]).reshape(head_g.shape)
    small = head_g.shape[1] // 4
    to_line(1, lambda other: head_g.at[:, pl.ds(pl.multiple_of(other * small, 8), small), :], head_zr)
    part, gain_six = norm_grads(z2[...], gain_d[2], dec_sum(2))
    grad_z = part
    up_low = grad_z.astype(LOW)
    wide[...] = dot_nn(up_low, dec[2])

    @pl.loop(0, strips)
    def _(i):
        slope = gelu_slope(u_d[strip_rows(i), :])
        gp_d[strip_rows(i), :] = (wide[strip_rows(i), :] * slope).astype(LOW)

    dec_pair(3, dot_nt(gp_d[...], dec[1]))
    low_g[1] = dot_tn(up_low, h_d[...]).astype(LOW).reshape(head_g.shape)
    low_g[0] = dot_tn(b_d[...], gp_d[...]).astype(LOW).reshape(head_g.shape)
    to_plane(1, lambda peer: low_g.at[:, peer], low_r)
    part, gain_five = norm_grads(z1[...], gain_d[1], dec_sum(3))
    grad_z = grad_z + part
    z2[...] = grad_z
    up_low = grad_z.astype(LOW)
    b_d[...] = up_low
    gp_d[...] = dot_nn(up_low, dec[0]).astype(LOW)

    @pl.loop(0, dec_heads)
    def _(h):
        slab = qkv_d[:, slab_of(h)]
        grad_mix = move(gp_d[:, slab_of(h)], 3, 2)
        s_d[...] = dot_nt(grad_mix, slab)

        @pl.loop(0, strips)
        def _(i):
            soft = p_d[h, strip_rows(i), :].astype(F32)
            grad = s_d[strip_rows(i), :]
            ds_d[strip_rows(i), :] = (
                soft * (grad - jnp.sum(grad * soft, axis=-1, keepdims=True))
            ).astype(LOW)

        query = move(qkv_d[own, slab_of(h)], 0, 1)
        grad_query = move((dot_nn(ds_d[...], slab) * SCALE).astype(LOW), 1, 0)
        s_d[:SLAB, :] = dot_tn(query, ds_d[...]) * SCALE
        s_d[:SLAB, :] += dot_tn(grad_mix, p_d[h])
        for q in range(4):
            g_d[q * tubes : (q + 1) * tubes, slab_of(h)] = (
                s_d[:SLAB, q * tubes : (q + 1) * tubes].T.astype(LOW)
            )
        g_d[own, slab_of(h)] = g_d[own, slab_of(h)] + grad_query

    attend_g[...] = dot_tn(b_d[...], mix_d[...]).reshape(head_g.shape)
    vec_g[...] = jnp.zeros_like(vec_g)

    def all_rows(q, carry):
        gain_four, mask_grad, latent_grad = carry
        attend_g[...] += dot_tn(a_all[block_rows(q), :], g_d[block_rows(q), :]).reshape(head_g.shape)
        narrow[...] = dot_nt(g_d[block_rows(q), :], dec[0])
        share_here = jnp.where(q == s, first_core, 0.0)

        def strip_grads(i, sums):
            rows = pl.ds(pl.multiple_of(q * tubes + i * strip, strip), strip)
            part, more = norm_grads(z_all[rows, :], gain_d[0], narrow[strip_rows(i), :])
            grad = part + z2[strip_rows(i), :] * share_here
            z1[strip_rows(i), :] = grad
            masked = jnp.sum(strip_hidden(q, i) * grad, axis=0, keepdims=True)
            return (sums[0] + more, sums[1] + masked)

        gain_four, mask_grad = lax.fori_loop(0, strips, strip_grads, (gain_four, mask_grad))
        lane = lax.broadcasted_iota(jnp.int32, (1, tubes), 1)
        ids = jnp.where(lane < real, q * real + lane, -7)
        picker = (vis_col[...] == ids).astype(F32).astype(LOW)
        return (gain_four, mask_grad, latent_grad + dot_nn(picker, z1[...].astype(LOW)))

    narrow = s_d.at[:, :width_d]
    row_zero = jnp.zeros((1, width_d), F32)
    gain_four, mask_grad, latent_grad = lax.fori_loop(
        0, 4, all_rows, (row_zero, row_zero, jnp.zeros((seen_rows, width_d), F32))
    )

    to_plane(2, lambda peer: attend_g.at[peer], attend_r)

    lat_a[...] = latent_grad.astype(LOW)
    send(lat_a, lat_got, pair_send.at[8], pair_recv.at[8], mate)
    wait_got(lat_got, pair_recv.at[8])
    lat_b[...] = (lat_a[...].astype(F32) + lat_got[...].astype(F32)).astype(LOW)
    half = seen_rows // 2
    mine = pl.ds(pl.multiple_of(t * half, 8), half)
    for k in (1, 2, 3):
        other = (s + k) % 4
        send(lat_b.at[mine, :], lat_z.at[k - 1], line_send.at[0, k - 1], line_recv.at[0, k - 1], {"seq": other})
    total = lat_b[mine, :].astype(F32)
    for k in (1, 2, 3):
        wait_got(lat_z.at[k - 1], line_recv.at[0, k - 1])
        total = total + lat_z[k - 1].astype(F32)
    lat_c[mine, :] = total.astype(LOW)
    send(lat_c.at[mine, :], lat_c.at[mine, :], pair_send.at[9], pair_recv.at[9], mate)
    wait_got(lat_c.at[mine, :], pair_recv.at[9])
    wait_got(lat_c.at[mine, :], pair_send.at[9])

    mine_z = pl.ds(pl.multiple_of(s * small, 8), small)
    head_z[...] = line_total(1, head_g[:, mine_z, :], head_zr)
    to_plane(0, lambda peer: head_z.at[peer], head_r)
    low_sum = plane_total(1, low_g[:, d].astype(F32), low_r)
    for q in range(4):
        low_z[q] = low_sum[:, q * small : (q + 1) * small, :].astype(LOW)
    to_line(2, lambda other: low_z.at[other], low_zr)

    grad_latent = lat_c[...]
    bor_g[:, :, PIX:] = dot_tn(c_e[:, :own_cols], grad_latent).reshape(4, rows, -1)
    grad_x, gain_three = norm_grads(x2[...], gain[2], dot_nt(grad_latent, bor[:, PIX:]))
    up_low = grad_x.astype(LOW)
    g_pre = (dot_nn(up_low, enc[2]) * u_e[...]).astype(LOW)
    enc_pair(2, dot_nt(g_pre, enc[1]))
    enc_low_g[1] = dot_tn(up_low[:, :own_cols], h_e[...]).astype(LOW).reshape(4, rows, -1)
    enc_low_g[0] = dot_tn(b_e[:, :own_cols], g_pre).astype(LOW).reshape(4, rows, -1)
    to_plane(3, lambda peer: enc_low_g.at[:, peer], enc_low_r)
    part, gain_two = norm_grads(x1[...], gain[1], enc_sum(2))
    grad_x = grad_x + part
    x2[...] = grad_x
    up_low = grad_x.astype(LOW)
    b_e[...] = up_low
    h_e[...] = dot_nn(up_low, enc[0]).astype(LOW)

    @pl.loop(0, enc_heads)
    def _(h):
        slab = qkv_e[:, slab_of(h)]
        grad_mix = h_e[:, slab_of(h)][:, 3 * HD :]
        soft = p_e[h].astype(F32)
        grad = dot_nt(grad_mix, slab[:, 2 * HD : 3 * HD])
        grad_scores = (soft * (grad - jnp.sum(grad * soft, axis=-1, keepdims=True))).astype(LOW)
        grad_query = (dot_nn(grad_scores, slab[:, HD : 2 * HD]) * SCALE).astype(LOW)
        grad_key = (dot_tn(grad_scores, slab[:, :HD]) * SCALE).astype(LOW)
        grad_value = dot_tn(p_e[h], grad_mix).astype(LOW)
        h_e[:, slab_of(h)] = jnp.concatenate(
            [grad_query, grad_key, grad_value, jnp.zeros((seen_rows, HD), LOW)], axis=1
        )

    enc_pair(3, dot_nt(h_e[...], enc[0]))
    enc_wide_g[...] = (
        dot_tn(b_e[:, :own_cols], mix_e[...]) + dot_tn(a_e[:, :own_cols], h_e[...])
    ).reshape(4, rows, -1)
    to_plane(4, lambda peer: enc_wide_g.at[peer], enc_wide_r)
    attend_sum = plane_total(2, attend_g[d], attend_r)
    for q in range(4):
        attend_z[q] = attend_sum[q * small : (q + 1) * small, :]
    to_line(3, lambda other: attend_z.at[other], attend_zr)
    part, gain_one = norm_grads(x0[...], gain[0], enc_sum(3))
    grad_x = x2[...] + part
    bor_g[:, :, :PIX] = dot_tn(grad_x[:, :own_cols].astype(LOW), seen[...]).reshape(4, rows, -1)
    half_rows = pl.ds(pl.multiple_of(t * part_rows, 8), part_rows)
    to_plane(5, lambda peer: bor_g.at[peer, half_rows, :], bor_r)

    vec_g[...] = jnp.zeros_like(vec_g)
    vec_g[0:1, :] = gain_one * 0.5
    vec_g[1:2, :] = gain_two * 0.5
    vec_g[2:3, :] = gain_three * 0.5
    vec_g[3:4, :width_d] = gain_four
    vec_g[4:5, :width_d] = gain_five * 0.5
    vec_g[5:6, :width_d] = gain_six * 0.5
    vec_g[6:7, :width_d] = mask_grad
    send(vec_g, vec_got, pair_send.at[10], pair_recv.at[10], mate)
    wait_got(vec_got, pair_recv.at[10])
    vec_p[...] = vec_g[...] + vec_got[...]
    to_plane(6, lambda peer: vec_p, vec_r)
    vec_z[...] = plane_total(6, vec_p[...], vec_r)
    to_line(4, lambda other: vec_z, vec_zr)

    def squares(value):
        return jnp.sum(value * value)

    low_total = line_total(2, low_z[s].astype(F32), low_zr)
    low_o[...] = low_total
    head_total = plane_total(0, head_z[d], head_r)
    head_o[...] = head_total
    square = squares(low_total) + squares(head_total)
    low_total = plane_total(3, enc_low_g[:, d].astype(F32), enc_low_r)
    enc_low_o[...] = low_total
    square = square + squares(low_total)
    attend_total = line_total(3, attend_z[s], attend_zr)
    attend_o[...] = attend_total
    square = square + squares(attend_total)
    wide_total = plane_total(4, enc_wide_g[d], enc_wide_r)
    enc_wide_o[...] = wide_total
    square = square + squares(wide_total)
    vec_line = line_total(4, jnp.zeros_like(vec_z), vec_zr)
    vec_row = lax.broadcasted_iota(jnp.int32, vec_z.shape, 0)
    vec_total = vec_z[...] + jnp.where(vec_row >= 3, vec_line, 0.0)
    vec_o[...] = vec_total
    bor_total = plane_total(5, bor_g[d, half_rows, :], bor_r)
    bor_o[half_rows, :] = bor_total
    send(bor_o.at[half_rows, :], bor_o.at[half_rows, :], pair_send.at[11], pair_recv.at[11], mate)
    square = square + squares(bor_total)

    lane = lax.broadcasted_iota(jnp.int32, micro.shape, 1)
    stat[0] = jnp.where(lane == 2, square, loss * micro[...])
    send(stat.at[0], stat_r.at[0], pair_send.at[12], pair_recv.at[12], mate)
    wait_got(stat_r.at[0], pair_recv.at[12])
    stat[1] = stat[0] + stat_r[0]
    to_plane(7, lambda peer: stat.at[1], stat_r.at[1:4])
    stat[2] = plane_total(7, stat[1], stat_r.at[1:4])
    to_line(5, lambda other: stat.at[2], stat_r.at[4:7])
    stat_o[...] = line_total(5, stat[2], stat_r.at[4:7]) + jnp.where(lane == 2, squares(vec_total), 0.0)

    for item, landing in enumerate(
        (head_r, low_r, attend_r, enc_low_r, enc_wide_r, bor_r, vec_r, stat_r.at[1:4])
    ):
        for j in range(3):
            wait_got(landing.at[j], plane_send.at[item, j])
    for item, landing in enumerate((lat_z, head_zr, low_zr, attend_zr, vec_zr, stat_r.at[4:7])):
        for k in range(3):
            wait_got(landing.at[k], line_send.at[item, k])
    for i in (2, 3):
        wait_got(enc_got.at[i % 2], pair_send.at[i])
        wait_got(dec_got.at[i % 2], pair_send.at[4 + i])
    wait_got(lat_got, pair_send.at[8])
    wait_got(vec_got, pair_send.at[10])
    wait_got(bor_o.at[half_rows, :], pair_send.at[11])
    wait_got(bor_o.at[half_rows, :], pair_recv.at[11])
    wait_got(stat_r.at[0], pair_send.at[12])


def run_step(enc, dec, bor, gains, seen, pixels, vis_col, vis_row, table, wgt, micro):
    v = pltpu.VMEM
    width, inner = enc.shape[1:]
    width_d, inner_d = dec.shape[1:]
    edge = bor.shape[1]
    tubes = pixels.shape[0]
    everyone = 4 * tubes
    seen_rows = vis_col.shape[0]
    rows = width // 16
    span = width_d // 4
    small = width_d // 16
    vmem = pl.BlockSpec(memory_space=pltpu.VMEM)
    shape = jax.ShapeDtypeStruct
    tile = (8, 128)
    return pl.pallas_call(
        step_kernel,
        out_shape=(
            shape((rows, inner), F32),
            shape((2, rows, inner), F32),
            shape((small, inner_d), F32),
            shape((2, small, inner_d), F32),
            shape((small, inner_d), F32),
            shape((rows, edge), F32),
            shape((8, width), F32),
            shape(tile, F32),
        ),
        in_specs=[vmem] * 11,
        out_specs=(vmem,) * 8,
        scratch_shapes=[
            v((seen_rows, width), F32), v((seen_rows, width), F32), v((seen_rows, width), F32),
            v((seen_rows, inner), LOW), v((seen_rows, inner), LOW),
            v((inner // SLAB, seen_rows, seen_rows), LOW),
            v((seen_rows, inner), F32),
            v((seen_rows, width), LOW), v((seen_rows, width), LOW), v((seen_rows, width), LOW),
            v((seen_rows, inner), LOW),
            v((everyone, width_d), F32), v((everyone, width_d), LOW), v((everyone, inner_d), LOW),
            v((inner_d // SLAB, tubes, everyone), LOW),
            v((tubes, everyone), F32), v((tubes, everyone), LOW),
            v((tubes, inner_d), LOW),
            v((tubes, width_d), F32), v((tubes, width_d), F32),
            v((tubes, inner_d), F32),
            v((tubes, width_d), LOW), v((tubes, inner_d), LOW), v((tubes, width_d), LOW),
            v((tubes, inner_d), LOW),
            v((everyone, inner_d), LOW),
            v((tubes, width_d), F32), v((tubes, width_d), F32),
            v((2, seen_rows, width_d), LOW),
            v((seen_rows, width_d), LOW), v((seen_rows, width_d), LOW), v((seen_rows, width_d), LOW),
            v((3, seen_rows // 2, width_d), LOW),
            v((seen_rows, width_d), LOW),
            v((2, seen_rows, width), LOW), v((2, seen_rows, width), LOW),
            v((2, tubes, width_d), LOW), v((2, tubes, width_d), LOW),
            v((8, width), F32), v((8, width), F32),
            v((4, rows, inner), F32), v((2, 4, rows, inner), LOW),
            v((4, span, inner_d), F32), v((2, 4, span, inner_d), LOW), v((4, span, inner_d), F32),
            v((4, rows, edge), F32),
            v((3, rows, inner), F32), v((3, 2, rows, inner), LOW),
            v((3, span, inner_d), F32), v((3, 2, span, inner_d), LOW), v((3, small, inner_d), F32),
            v((3, rows // 2, edge), F32), v((3, 8, width), F32),
            v((4, small, inner_d), F32), v((3, 4, small, inner_d), F32),
            v((4, small, inner_d), F32), v((3, small, inner_d), F32),
            v((4, 2, small, inner_d), LOW), v((3, 2, small, inner_d), LOW),
            v((8, width), F32), v((3, 8, width), F32), v((8, width), F32),
            v((3,) + tile, F32), v((7,) + tile, F32),
            pltpu.SemaphoreType.DMA((13,)), pltpu.SemaphoreType.DMA((13,)),
            pltpu.SemaphoreType.DMA((6, 3)), pltpu.SemaphoreType.DMA((6, 3)),
            pltpu.SemaphoreType.DMA((8, 3)), pltpu.SemaphoreType.DMA((8, 3)),
        ],
        compiler_params=pltpu.CompilerParams(
            collective_id=1, has_side_effects=True, vmem_limit_bytes=67043328
        ),
        name="run_step",
    )(enc, dec, bor, gains, seen, pixels, vis_col, vis_row, table, wgt, micro)


def layer_norm(x, norm_gain):
    row_mean = jnp.mean(x, axis=-1, keepdims=True)
    centred = x - row_mean
    variance = jnp.mean(centred * centred, axis=-1, keepdims=True)
    return centred * lax.rsqrt(variance + EPS_NORM) * norm_gain


def sinusoid(positions, model_width):
    half_width = model_width // 2
    frequency = jnp.exp(
        jnp.arange(half_width, dtype=jnp.float32) * (-math.log(10000.0) / half_width)
    )
    angles = positions.astype(jnp.float32)[:, None] * frequency[None, :]
    return jnp.concatenate([jnp.sin(angles), jnp.cos(angles)], axis=1)


def gelu_exact(v):
    return jax.nn.gelu(v, approximate=False)


def softmax_rows(scores):
    return jax.nn.softmax(scores, axis=-1)


def tensor_total(value):
    return lax.psum(value.astype(jnp.bfloat16), "tensor").astype(jnp.float32)


def gather_weights(encoder_weights, decoder_weights, border_weights, vector_params):
    return (
        lax.all_gather(encoder_weights, ("dp", "seq"), axis=1, tiled=True),
        lax.all_gather(decoder_weights, ("dp", "seq"), axis=1, tiled=True),
        lax.all_gather(border_weights, ("dp", "seq"), axis=0, tiled=True),
        lax.all_gather(vector_params, ("dp", "seq"), axis=0, tiled=True),
    )


def attend_forward(x, blocks, norm_gain, across):
    scale = blocks.shape[-1] ** (-0.5)
    normed, norm_back = jax.vjp(layer_norm, x, norm_gain)
    normed_low = normed.astype(jnp.bfloat16)
    projected = jnp.einsum(
        "td,dhce->chte", normed_low, blocks[:, :, :3, :], preferred_element_type=jnp.float32
    ).astype(jnp.bfloat16)
    query_rows = projected[0]
    key_rows = projected[1]
    value_rows = projected[2]
    if across:
        key_rows, value_rows = (
            lax.all_gather(key_rows, "seq", axis=1, tiled=True),
            lax.all_gather(value_rows, "seq", axis=1, tiled=True),
        )
    scores = (
        jnp.einsum("hte,hse->hts", query_rows, key_rows, preferred_element_type=jnp.float32) * scale
    )
    softmaxed, soft_back = jax.vjp(softmax_rows, scores)
    soft_low = softmaxed.astype(jnp.bfloat16)
    mixture = jnp.einsum(
        "hts,hse->hte", soft_low, value_rows, preferred_element_type=jnp.float32
    ).astype(jnp.bfloat16)
    branch = jnp.einsum(
        "hte,dhe->td", mixture, blocks[:, :, 3, :], preferred_element_type=jnp.float32
    )
    kept = (normed_low, query_rows, key_rows, value_rows, soft_low, soft_back, mixture, norm_back)
    return (x + tensor_total(branch), kept)


def attend_backward(upstream, blocks, kept, across):
    scale = blocks.shape[-1] ** (-0.5)
    normed_low, query_rows, key_rows, value_rows, soft_low, soft_back, mixture, norm_back = kept
    upstream_low = upstream.astype(jnp.bfloat16)
    grad_mixture = jnp.einsum(
        "td,dhe->hte", upstream_low, blocks[:, :, 3, :], preferred_element_type=jnp.float32
    ).astype(jnp.bfloat16)
    grad_output_w = jnp.einsum(
        "hte,td->dhe", mixture, upstream_low, preferred_element_type=jnp.float32
    )
    grad_soft = jnp.einsum(
        "hte,hse->hts", grad_mixture, value_rows, preferred_element_type=jnp.float32
    )
    grad_scores = soft_back(grad_soft)[0].astype(jnp.bfloat16)
    grad_query = (
        jnp.einsum("hts,hse->hte", grad_scores, key_rows, preferred_element_type=jnp.float32)
        * scale
    ).astype(jnp.bfloat16)
    grad_key = (
        jnp.einsum("hts,hte->hse", grad_scores, query_rows, preferred_element_type=jnp.float32)
        * scale
    )
    grad_value = jnp.einsum(
        "hts,hte->hse", soft_low, grad_mixture, preferred_element_type=jnp.float32
    )
    if across:
        grad_key, grad_value = (
            lax.psum_scatter(
                grad_key.astype(jnp.bfloat16), "seq", scatter_dimension=1, tiled=True
            ).astype(jnp.float32),
            lax.psum_scatter(
                grad_value.astype(jnp.bfloat16), "seq", scatter_dimension=1, tiled=True
            ).astype(jnp.float32),
        )
    grad_projected = jnp.stack(
        [grad_query, grad_key.astype(jnp.bfloat16), grad_value.astype(jnp.bfloat16)]
    )
    grad_input_w = jnp.einsum(
        "td,chte->dhce", normed_low, grad_projected, preferred_element_type=jnp.float32
    )
    grad_normed = tensor_total(
        jnp.einsum(
            "chte,dhce->td", grad_projected, blocks[:, :, :3, :], preferred_element_type=jnp.float32
        )
    )
    grad_x, grad_gain = norm_back(grad_normed)
    weight_grad = jnp.concatenate([grad_input_w, grad_output_w[:, :, None, :]], axis=2)
    return (upstream + grad_x, weight_grad, grad_gain)


def feed_forward_forward(x, up_proj, down_proj, norm_gain):
    normed, norm_back = jax.vjp(layer_norm, x, norm_gain)
    normed_low = normed.astype(jnp.bfloat16)
    preact = jnp.dot(normed_low, up_proj, preferred_element_type=jnp.float32)
    activation, gelu_back = jax.vjp(gelu_exact, preact)
    activation_low = activation.astype(jnp.bfloat16)
    branch = jnp.einsum("tf,df->td", activation_low, down_proj, preferred_element_type=jnp.float32)
    return (x + tensor_total(branch), (normed_low, activation_low, gelu_back, norm_back))


def feed_forward_backward(upstream, up_proj, down_proj, kept):
    normed_low, activation_low, gelu_back, norm_back = kept
    upstream_low = upstream.astype(jnp.bfloat16)
    grad_activation = jnp.dot(upstream_low, down_proj, preferred_element_type=jnp.float32)
    grad_down = jnp.einsum(
        "td,tf->df", upstream_low, activation_low, preferred_element_type=jnp.float32
    )
    grad_preact = gelu_back(grad_activation)[0].astype(jnp.bfloat16)
    grad_up = jnp.einsum("td,tf->df", normed_low, grad_preact, preferred_element_type=jnp.float32)
    grad_normed = tensor_total(
        jnp.einsum("tf,df->td", grad_preact, up_proj, preferred_element_type=jnp.float32)
    )
    grad_x, grad_gain = norm_back(grad_normed)
    return (upstream + grad_x, jnp.stack([grad_up, grad_down]), grad_gain)


def clip_step(clip_pixels, visible_row, weight, gathered):
    encoder_full, decoder_full, border_full, vector_full = gathered
    local_tubes = clip_pixels.shape[0]
    encoder_heads = encoder_full.shape[2] // (4 * HD)
    decoder_heads = decoder_full.shape[2] // (4 * HD)
    encoder_blocks = encoder_full[0].reshape(D, encoder_heads, 4, HD)
    decoder_blocks = decoder_full[0].reshape(DD, decoder_heads, 4, HD)
    vector_float = vector_full.astype(jnp.float32)
    width_ratio = D // DD
    gain_list = [
        vector_float[:, 0:width_ratio].reshape(D),
        vector_float[:, width_ratio : 2 * width_ratio].reshape(D),
        vector_float[:, 2 * width_ratio : 3 * width_ratio].reshape(D),
        vector_float[:, 3 * width_ratio],
        vector_float[:, 3 * width_ratio + 1],
        vector_float[:, 3 * width_ratio + 2],
    ]
    mask_token = vector_float[:, 3 * width_ratio + 3]
    patch_proj = border_full[:, :PIX]
    latent_proj = border_full[:, PIX:]
    pixel_head = decoder_full[3]
    tube_ids = lax.axis_index("seq") * local_tubes + jnp.arange(local_tubes, dtype=jnp.int32)
    picked = tube_ids[:, None] == visible_row[None, :]
    picked_low = picked.astype(jnp.bfloat16)
    picked_float = picked.astype(jnp.float32)
    hidden_mask = 1.0 - jnp.sum(picked_float, axis=1)
    selected = jnp.einsum("tv,tp->vp", picked_low, clip_pixels, preferred_element_type=jnp.float32)
    seen_pixels = lax.psum(selected.astype(jnp.bfloat16), "seq")
    x = jnp.einsum(
        "vp,dp->vd", seen_pixels, patch_proj, preferred_element_type=jnp.float32
    ) + sinusoid(visible_row, D)
    x, enc_attend_kept = attend_forward(x, encoder_blocks, gain_list[0], False)
    x, enc_feed_kept = feed_forward_forward(x, encoder_full[1], encoder_full[2], gain_list[1])
    encoded, encoded_back = jax.vjp(layer_norm, x, gain_list[2])
    encoded_low = encoded.astype(jnp.bfloat16)
    latent = jnp.dot(encoded_low, latent_proj, preferred_element_type=jnp.float32)
    z = (
        jnp.dot(picked_float, latent, precision=HIGH)
        + hidden_mask[:, None] * mask_token[None, :]
        + sinusoid(tube_ids, DD)
    )
    z, dec_attend_kept = attend_forward(z, decoder_blocks, gain_list[3], True)
    z, dec_feed_kept = feed_forward_forward(z, decoder_full[1], decoder_full[2], gain_list[4])
    final_norm, final_back = jax.vjp(layer_norm, z, gain_list[5])
    final_low = final_norm.astype(jnp.bfloat16)
    prediction = jnp.dot(final_low, pixel_head, preferred_element_type=jnp.float32)
    pixel_share = pixel_head.shape[1]
    target = lax.dynamic_slice_in_dim(
        clip_pixels, lax.axis_index("tensor") * pixel_share, pixel_share, 1
    ).astype(jnp.float32)
    residue = prediction - target
    loss_part = weight * jnp.sum(hidden_mask[:, None] * residue * residue)
    grad_prediction = (weight * 2.0 * hidden_mask[:, None] * residue).astype(jnp.bfloat16)
    grad_head = jnp.einsum(
        "td,tp->dp", final_low, grad_prediction, preferred_element_type=jnp.float32
    )
    grad_final = tensor_total(
        jnp.einsum("tp,dp->td", grad_prediction, pixel_head, preferred_element_type=jnp.float32)
    )
    grad_z, grad_gain_six = final_back(grad_final)
    grad_z, grad_dec_feed, grad_gain_five = feed_forward_backward(
        grad_z, decoder_full[1], decoder_full[2], dec_feed_kept
    )
    grad_z, grad_dec_attend, grad_gain_four = attend_backward(
        grad_z, decoder_blocks, dec_attend_kept, True
    )
    grad_mask = jnp.sum(hidden_mask[:, None] * grad_z, axis=0)
    latent_part = jnp.dot(picked_float.T, grad_z, precision=HIGH)
    grad_latent = lax.psum(latent_part.astype(jnp.bfloat16), "seq")
    grad_latent_proj = jnp.einsum(
        "vd,ve->de", encoded_low, grad_latent, preferred_element_type=jnp.float32
    )
    grad_encoded = jnp.einsum(
        "ve,de->vd", grad_latent, latent_proj, preferred_element_type=jnp.float32
    )
    grad_x, grad_gain_three = encoded_back(grad_encoded)
    grad_x, grad_enc_feed, grad_gain_two = feed_forward_backward(
        grad_x, encoder_full[1], encoder_full[2], enc_feed_kept
    )
    grad_x, grad_enc_attend, grad_gain_one = attend_backward(
        grad_x, encoder_blocks, enc_attend_kept, False
    )
    grad_patch = jnp.einsum(
        "vd,vp->dp", grad_x.astype(jnp.bfloat16), seen_pixels, preferred_element_type=jnp.float32
    )
    encoder_grad = jnp.stack([grad_enc_attend.reshape(D, -1), grad_enc_feed[0], grad_enc_feed[1]])
    decoder_grad = jnp.stack(
        [grad_dec_attend.reshape(DD, -1), grad_dec_feed[0], grad_dec_feed[1], grad_head]
    )
    border_grad = jnp.concatenate([grad_patch, grad_latent_proj], axis=1)
    vector_grad = jnp.concatenate(
        [
            grad_gain_one.reshape(DD, width_ratio),
            grad_gain_two.reshape(DD, width_ratio),
            grad_gain_three.reshape(DD, width_ratio),
            grad_gain_four[:, None],
            grad_gain_five[:, None],
            grad_gain_six[:, None],
            grad_mask[:, None],
        ],
        axis=1,
    )
    return (loss_part, (encoder_grad, decoder_grad, border_grad, vector_grad))


def adam_update(gradient, weights, mean_old, square_old, factor):
    scaled = gradient * factor
    mean_next = BETA_FIRST * mean_old + (1.0 - BETA_FIRST) * scaled
    square_next = BETA_SECOND * square_old + (1.0 - BETA_SECOND) * scaled * scaled
    first_fix = 1.0 - BETA_FIRST**BIAS_STEP
    second_fix = 1.0 - BETA_SECOND**BIAS_STEP
    update = -LEARN_RATE * (
        mean_next / first_fix / (jnp.sqrt(square_next / second_fix) + ADAM_EPS)
        + WEIGHT_DECAY * weights.astype(jnp.float32)
    )
    return (mean_next, square_next, update)


def local(
    pixels,
    visible,
    micro_of,
    encoder_weights,
    decoder_weights,
    border_weights,
    vector_params,
    encoder_mean,
    decoder_mean,
    border_mean,
    vector_mean,
    encoder_square,
    decoder_square,
    border_square,
    vector_square,
):
    clips_here = pixels.shape[0]
    seq_count = lax.axis_size("seq")
    dp_count = lax.axis_size("dp")
    tensor_count = lax.axis_size("tensor")
    seq_here = lax.axis_index("seq")
    micro_slots = jnp.arange(MICRO, dtype=jnp.int32)
    counts = jnp.sum((micro_of[:, None] == micro_slots[None, :]).astype(jnp.float32), axis=0)
    gathered = gather_weights(encoder_weights, decoder_weights, border_weights, vector_params)
    clip_index = lax.axis_index("dp") * clips_here + 0
    micro_index = micro_of[clip_index]
    weight = 1.0 / (counts[micro_index] * float(MICRO * (TUBES - VIS) * PIX))
    loss_part, clip_grads = clip_step(pixels[0], visible[0], weight, gathered)
    losses = loss_part * (micro_slots == micro_index).astype(jnp.float32)
    flat_count = dp_count * seq_count
    small_rows = clip_grads[3].shape[0]
    small_block = small_rows // flat_count
    small_ids = jnp.arange(small_rows, dtype=jnp.int32)
    column_ids = jnp.arange(clip_grads[3].shape[1], dtype=jnp.int32)
    small_keep = (small_ids // small_block % seq_count == seq_here).astype(jnp.float32)
    vector_keep = jnp.where(column_ids[None, :] < 3 * (D // DD), small_keep[:, None], 1.0)
    vector_total = clip_grads[3] * vector_keep
    row_ids = jnp.arange(D, dtype=jnp.int32)
    row_keep = (row_ids // (D // flat_count) % seq_count == seq_here).astype(jnp.float32)
    summed = (
        lax.psum_scatter(
            clip_grads[0] * row_keep[None, :, None], ("dp", "seq"), scatter_dimension=1, tiled=True
        ),
        lax.psum_scatter(clip_grads[1], ("dp", "seq"), scatter_dimension=1, tiled=True),
        lax.psum_scatter(
            clip_grads[2] * row_keep[:, None], ("dp", "seq"), scatter_dimension=0, tiled=True
        ),
        lax.psum_scatter(vector_total, ("dp", "seq"), scatter_dimension=0, tiled=True),
    )
    square_sum = (
        jnp.sum(summed[0] * summed[0])
        + jnp.sum(summed[1] * summed[1])
        + (jnp.sum(summed[2] * summed[2]) + jnp.sum(summed[3] * summed[3])) / tensor_count
    )
    losses_all, square_all = lax.psum((losses, square_sum), ("dp", "seq", "tensor"))
    grad_norm = jnp.sqrt(square_all)
    factor = jnp.minimum(1.0, CLIP_LIMIT / grad_norm)
    enc_next = adam_update(summed[0], encoder_weights, encoder_mean, encoder_square, factor)
    dec_next = adam_update(summed[1], decoder_weights, decoder_mean, decoder_square, factor)
    bor_next = adam_update(summed[2], border_weights, border_mean, border_square, factor)
    vec_next = adam_update(summed[3], vector_params, vector_mean, vector_square, factor)
    return (
        enc_next[0],
        enc_next[1],
        enc_next[2],
        dec_next[0],
        dec_next[1],
        dec_next[2],
        bor_next[0],
        bor_next[1],
        bor_next[2],
        vec_next[0],
        vec_next[1],
        vec_next[2],
        losses_all,
        jnp.reshape(grad_norm, (1,)),
    )


def fits_fast(mesh):
    return dict(mesh.shape) == {"dp": 4, "seq": 4, "tensor": 2}


def turned(values, s, rows):
    blocks = values.reshape((4, 4, rows) + values.shape[1:])
    return jnp.swapaxes(jnp.roll(blocks, -s, axis=1), 0, 1).reshape(values.shape)


def fast_local(
    pixels,
    visible,
    micro_of,
    encoder_weights,
    decoder_weights,
    border_weights,
    vector_params,
    encoder_mean,
    decoder_mean,
    border_mean,
    vector_mean,
    encoder_square,
    decoder_square,
    border_square,
    vector_square,
):
    low = jnp.bfloat16
    clip_pixels = pixels[0]
    visible_row = visible[0]
    s = lax.axis_index("seq")
    rows = encoder_weights.shape[1]
    small = decoder_weights.shape[1]
    own = 4 * rows
    micro_slots = jnp.arange(MICRO, dtype=jnp.int32)
    counts = jnp.sum((micro_of[:, None] == micro_slots[None, :]).astype(jnp.float32), axis=0)
    micro_index = micro_of[lax.axis_index("dp")]
    weight = 1.0 / (counts[micro_index] * float(MICRO * (TUBES - VIS) * PIX))
    local_tubes = clip_pixels.shape[0]
    tube_ids = s * local_tubes + jnp.arange(local_tubes, dtype=jnp.int32)
    picked = tube_ids[:, None] == visible_row[None, :]
    picked_float = picked.astype(jnp.float32)
    hidden_mask = 1.0 - jnp.sum(picked_float, axis=1)
    selected = jnp.einsum(
        "tv,tp->vp", picked.astype(low), clip_pixels, preferred_element_type=jnp.float32
    ).astype(low)
    own_vectors = vector_params.astype(jnp.float32)
    ratio = D // DD
    lines = [own_vectors[:, ratio * i : ratio * (i + 1)].reshape(1, rows) for i in range(3)]
    lines += [
        jnp.pad(own_vectors[:, 3 * ratio + i].reshape(1, small), ((0, 0), (0, rows - small)))
        for i in range(4)
    ]
    tile = jnp.pad(jnp.concatenate(lines), ((0, 1), (0, 128 - rows)))
    encoder_full, decoder_full, border_full, vector_tiles, pixel_parts = gather_all(
        encoder_weights, decoder_weights, border_weights, tile, jnp.pad(selected, ((0, 3), (0, 0)))
    )
    gains = [turned(vector_tiles[:, i, :rows].reshape(D), s, rows) for i in range(3)]
    gains += [vector_tiles[:, 3 + i, :small].reshape(DD) for i in range(4)]
    rows_of = [g[None, :] for g in gains[:3]] + [
        jnp.pad(g, (0, D - DD))[None, :] for g in gains[3:]
    ]
    gain_rows = jnp.pad(jnp.concatenate(rows_of), ((0, 1), (0, 0)))
    column = turned(jnp.arange(D, dtype=jnp.int32), s, rows)
    half_d, half_dd = D // 2, DD // 2
    column_d = jnp.arange(D, dtype=jnp.int32)
    table = jnp.stack(
        [
            jnp.exp((column % half_d).astype(jnp.float32) * (-math.log(10000.0) / half_d)),
            (column >= half_d).astype(jnp.float32),
            jnp.exp((column_d % half_dd).astype(jnp.float32) * (-math.log(10000.0) / half_dd)),
            (column_d >= half_dd).astype(jnp.float32),
        ]
    )
    table = jnp.pad(table, ((0, 4), (0, 0)))
    padded = jnp.pad(visible_row, (0, 3), constant_values=-1)
    share = decoder_weights.shape[2]
    own_pixels = lax.dynamic_slice_in_dim(
        clip_pixels, lax.axis_index("tensor") * share, share, 1
    )
    lane = jnp.arange(128, dtype=jnp.int32)
    enc_first, enc_later, attend_sum, low_sum, head_sum, border_sum, vector_sum, stats = run_step(
        encoder_full,
        decoder_full,
        border_full,
        gain_rows,
        jnp.sum(pixel_parts.astype(jnp.float32), axis=0).astype(low),
        jnp.pad(own_pixels, ((0, -local_tubes % 32), (0, 0))),
        padded[:, None],
        padded[None, :],
        table,
        jnp.full((8, 128), weight, jnp.float32),
        jnp.broadcast_to((lane == micro_index).astype(jnp.float32), (8, 128)),
    )
    enc_sum = jnp.concatenate([enc_first[None], enc_later])
    dec_sum = jnp.concatenate([attend_sum[None], low_sum, head_sum[None]])
    d = lax.axis_index("dp")
    first_rows = lax.dynamic_slice(vector_sum, (0, d * rows), (3, rows))
    later_rows = lax.dynamic_slice(vector_sum, (3, (d * 4 + s) * small), (4, small))
    vector_own = jnp.concatenate(
        [first_rows[i].reshape(small, ratio) for i in range(3)] + [later_rows.T], axis=1
    )
    grad_norm = jnp.sqrt(stats[0, 2])
    factor = jnp.minimum(1.0, CLIP_LIMIT / grad_norm)
    enc_next = adam_update(enc_sum, encoder_weights, encoder_mean, encoder_square, factor)
    dec_next = adam_update(dec_sum, decoder_weights, decoder_mean, decoder_square, factor)
    bor_next = adam_update(border_sum, border_weights, border_mean, border_square, factor)
    vec_next = adam_update(vector_own, vector_params, vector_mean, vector_square, factor)
    return (
        *enc_next,
        *dec_next,
        *bor_next,
        *vec_next,
        stats[0, :MICRO],
        jnp.reshape(grad_norm, (1,)),
    )


def solution(mesh):
    in_specs = (
        P("dp", "seq", None),
        P("dp", None),
        P(),
        P(None, ("dp", "seq"), "tensor"),
        P(None, ("dp", "seq"), "tensor"),
        P(("dp", "seq"), None),
        P(("dp", "seq"), None),
        P(None, ("dp", "seq"), "tensor"),
        P(None, ("dp", "seq"), "tensor"),
        P(("dp", "seq"), None),
        P(("dp", "seq"), None),
        P(None, ("dp", "seq"), "tensor"),
        P(None, ("dp", "seq"), "tensor"),
        P(("dp", "seq"), None),
        P(("dp", "seq"), None),
    )
    out_specs = (
        P(None, ("dp", "seq"), "tensor"),
        P(None, ("dp", "seq"), "tensor"),
        P(None, ("dp", "seq"), "tensor"),
        P(None, ("dp", "seq"), "tensor"),
        P(None, ("dp", "seq"), "tensor"),
        P(None, ("dp", "seq"), "tensor"),
        P(("dp", "seq"), None),
        P(("dp", "seq"), None),
        P(("dp", "seq"), None),
        P(("dp", "seq"), None),
        P(("dp", "seq"), None),
        P(("dp", "seq"), None),
        P(),
        P(),
    )
    chosen = fast_local if fits_fast(mesh) else local
    return jax.shard_map(chosen, mesh=mesh, in_specs=in_specs, out_specs=out_specs, check_vma=False)
```
